32 devices in a mesh: lvl: 8 (over z, y), lon: 4 (over x, core).
Axes of the slice: x: 2, y: 2, z: 4, core: 2. Of those that a mesh axis runs over, the one named last changes fastest.
Arguments:
- window: float32 [8, 16, 69, 512], P('lvl', None, None, 'lon'), may hold values from -6 to 6
- anchor: float32 [16, 69, 512], P(None, None, 'lon'), may hold values from -6 to 6
- noise: float32 [8, 16, 69, 512], P('lvl', None, None, 'lon'), may hold values from -6 to 6
- conv_in: bfloat16 [3, 3, 192, 69], replicated, may hold values from -0.25 to 0.25
- conv_out: bfloat16 [3, 3, 69, 192], replicated, may hold values from -0.15625 to 0.15625
- time_shift: float32 [192], replicated, may hold values from -4 to 4
- plan: int32 [256], replicated, may hold values from 0 to 999, as said below
- start: int32 [1], replicated, may hold values from 0 to 247
Outputs:
- advanced: float32 [8, 16, 69, 512], P('lvl', None, None, 'lon')
The draws below stay inside these ranges and needn't reach their ends.
Inputs may be any that keep to these rules, and one draw needn't show every extreme that they name: `plan`: strictly decreasing, first entry 999.
All inputs are finite; a program needn't handle non-finite values.
Results may differ from the reference program's by a relative error of at most 0.0003.
Values may be sent and summed in bfloat16 or wider, within the bound.
No kernel may reach another device: no remote copies, remote signals or barrier semaphores. Data moves between devices by JAX's collectives and lax.ppermute only.
A program may use at most 64 MiB of HBM per device.

```python
import jax
import jax.numpy as jnp

CIN = 69
HID = 192
LAT = 16
SWEEPS = 2
TABLE = 256
LEVELS = 8
LON = 512


def draw_plan(key, part):
    gaps = jax.random.randint(key, (TABLE,), 1, 4)
    return (999 - (jnp.cumsum(gaps) - gaps[0])).astype(jnp.int32)


def level_of(key, extent, split, least, high):
    def one(dim, shards_of):
        heights = jax.random.uniform(jax.random.fold_in(jax.random.fold_in(key, 6), dim), (shards_of,), jnp.float32, least / len(split), high / len(split))
        return jnp.repeat(jnp.exp(heights), extent[dim] // shards_of).reshape((-1,) + (1,) * (len(extent) - dim - 1))

    level = one(*split[0])
    for cut in split[1:]:
        level = level * one(*cut)
    return level


def normal_values(key, extent, deviation, bound, split=(), dtype=jnp.bfloat16):
    result = jax.random.normal(key, extent, jnp.float32) * deviation
    if len(split) > 0:
        result = level_of(key, extent, split, -0.22, 0.18) * result
    return jnp.clip(result, min=-bound, max=bound).astype(dtype)


def setup_inputs(seed: int = 0) -> dict:
    seeds = jax.random.split(jax.random.key(seed), 9)
    return {
        "window": normal_values(seeds[0], (LEVELS, LAT, CIN, LON), 1.0, 6.0, ((0, 8), (3, 4)), jnp.float32),
        "anchor": normal_values(seeds[1], (LAT, CIN, LON), 1.0, 6.0, ((2, 4),), jnp.float32),
        "noise": normal_values(seeds[2], (LEVELS, LAT, CIN, LON), 1.0, 6.0, ((0, 8), (3, 4)), jnp.float32),
        "conv_in": normal_values(seeds[3], (3, 3, HID, CIN), (9 * CIN) ** -0.5, 0.25),
        "conv_out": normal_values(seeds[4], (3, 3, CIN, HID), (9 * HID) ** -0.5, 0.15625),
        "time_shift": normal_values(seeds[5], (HID,), 1.0, 4.0, (), jnp.float32),
        "plan": draw_plan(jax.random.fold_in(seeds[8], 71), 0),
        "start": jax.random.randint(seeds[7], (1,), 0, TABLE - LEVELS).astype(jnp.int32),
    }


def convolve(field, weight):
    wrapped = jnp.concatenate([field[:, :, -1:], field, field[:, :, :1]], axis=2)
    padded = jnp.pad(wrapped, ((1, 1), (0, 0), (0, 0)))
    rows = field.shape[0]
    cols = field.shape[2]
    total = jnp.zeros((rows, weight.shape[2], cols), jnp.float32)
    for a in range(3):
        for b in range(3):
            piece = padded[a:a + rows, :, b:b + cols].astype(jnp.float32)
            total = total + jnp.einsum('oc,lcn->lon', weight[a, b].astype(jnp.float32), piece)
    return total

def reference(window, anchor, noise, conv_in, conv_out, time_shift, plan, start):
    first = start[0]
    times = jax.lax.dynamic_slice(plan, (first,), (LEVELS + 1,)).astype(jnp.float32)
    t_now = times[:-1]
    t_next = times[1:]
    beta = 0.1 + 19.9 * t_now / 1000.0
    step = (t_now - t_next) / 1000.0
    states = window
    inclusive = None
    for sweep in range(SWEEPS):
        incs = []
        for level in range(LEVELS):
            state = states[level]
            xb = state.astype(jnp.bfloat16)
            pre = convolve(xb, conv_in)
            hidden = jax.nn.silu(pre + t_now[level] / 1000.0 * time_shift[None, :, None]).astype(jnp.bfloat16)
            score = convolve(hidden, conv_out)
            inc = (0.5 * beta[level] * state + beta[level] * score) * step[level] + jnp.sqrt(beta[level] * step[level]) * noise[level]
            incs.append(inc)
        incs = jnp.stack(incs)
        inclusive = jnp.cumsum(incs, axis=0)
        states = anchor[None] + (inclusive - incs)
    return anchor[None] + inclusive
```

```python
import functools

import jax
import jax.numpy as jnp
from jax import lax
from jax.experimental import pallas as pl
from jax.experimental.pallas import tpu as pltpu
from jax.sharding import PartitionSpec as P

GROUP = 4
EDGE = 4
ROWS = 8
PACK = 16

VM = pl.BlockSpec(memory_space=pltpu.VMEM)
SM = pl.BlockSpec(memory_space=pltpu.SMEM)
F32 = jnp.float32
BF16 = jnp.bfloat16


def up_to(value, unit):
    return -(-value // unit) * unit


def call(kernel, outs, specs, scratch, flops):
    return pl.pallas_call(
        kernel,
        out_shape=[jax.ShapeDtypeStruct(shape, F32) for shape in outs],
        in_specs=specs,
        out_specs=[VM] * len(outs),
        scratch_shapes=scratch,
        cost_estimate=pl.CostEstimate(flops=flops, bytes_accessed=4 << 20, transcendentals=0),
    )


def edges_kernel(lat, win_ref, noise_ref, anchor_ref, first_ref, last_ref):
    chans = win_ref.shape[0] // lat
    width = win_ref.shape[1]
    firsts = []
    lasts = []
    for l in range(lat):
        rows = pl.ds(l, chans, stride=lat)
        win = win_ref[rows, :]
        noise = noise_ref[rows, :]
        anchor = anchor_ref[rows, :]
        firsts += [win[:, :4], noise[:, :2], anchor[:, :2]]
        lasts += [win[:, width - 4 :], noise[:, width - 2 :], anchor[:, width - 2 :]]
    first_ref[0:chans, :] = jnp.concatenate(firsts, axis=1)
    last_ref[0:chans, :] = jnp.concatenate(lasts, axis=1)


def lat_shifted(x, strip, pitch):
    size = x.shape[1]
    lane = lax.rem(lax.broadcasted_iota(jnp.int32, x.shape, 1), strip)
    below = jnp.where(lane < pitch, 0.0, pltpu.roll(x, pitch, 1))
    above = jnp.where(lane >= strip - pitch, 0.0, pltpu.roll(x, size - pitch, 1))
    return below, above


def score_of(x, shift, w_in_ref, w_out_ref, strip, pitch):
    size = x.shape[1]
    hid = w_in_ref.shape[0] // 3
    rows = w_out_ref.shape[0] // 9
    below, above = lat_shifted(x, strip, pitch)
    stacked = jnp.concatenate([below, x, above], axis=0).astype(BF16)
    taps = jnp.dot(w_in_ref[...], stacked, preferred_element_type=F32)
    pre = taps[hid : 2 * hid] + pltpu.roll(taps[:hid], 1, 1) + pltpu.roll(taps[2 * hid :], size - 1, 1)
    value = pre + shift
    hidden = (value / (1.0 + jnp.exp(-value))).astype(BF16)
    out = jnp.dot(w_out_ref[...], hidden, preferred_element_type=F32)
    lines = []
    for a in range(3):
        left = out[(3 * a) * rows : (3 * a + 1) * rows]
        mid = out[(3 * a + 1) * rows : (3 * a + 2) * rows]
        right = out[(3 * a + 2) * rows : (3 * a + 3) * rows]
        lines.append(mid + pltpu.roll(left, 1, 1) + pltpu.roll(right, size - 1, 1))
    below, _ = lat_shifted(lines[0], strip, pitch)
    _, above = lat_shifted(lines[2], strip, pitch)
    return lines[1] + below + above


def first_kernel(
    lat, me_ref, coef_ref, win_ref, noise_ref, before_ref, after_ref, shift_ref, w_in_ref, w_out_ref,
    *refs,
):
    outs = refs[:GROUP]
    waves = refs[GROUP : 2 * GROUP]
    x_ref, u_ref, inc_ref, wave_ref = refs[2 * GROUP :]
    chans = win_ref.shape[0] // lat
    width = win_ref.shape[1]
    sub = width // GROUP
    pitch = sub + 2 * EDGE
    strip = lat * pitch
    me = me_ref[0]
    half, drift, spread = coef_ref[0], coef_ref[1], coef_ref[2]
    x_ref[...] = jnp.zeros_like(x_ref)
    u_ref[...] = jnp.zeros_like(u_ref)
    blank = jnp.zeros((chans, 2), F32)
    for l in range(lat):
        rows = pl.ds(l, chans, stride=lat)
        win = win_ref[rows, :]
        noise = noise_ref[rows, :] * spread
        low = before_ref[0:chans, 8 * l : 8 * l + 8]
        high = after_ref[0:chans, 8 * l : 8 * l + 8]
        wide = jnp.concatenate([low[:, :4], win, high[:, :4]], axis=1)
        other = jnp.concatenate([blank, low[:, 4:6] * spread, noise, high[:, 4:6] * spread, blank], axis=1)
        total = wide * half + other
        for q in range(GROUP):
            lanes = slice(q * strip + l * pitch, q * strip + (l + 1) * pitch)
            x_ref[0:chans, lanes] = wide[:, q * sub : q * sub + pitch]
            u_ref[0:chans, lanes] = total[:, q * sub : q * sub + pitch]
            wave_ref[q, 0:chans, l * sub : (l + 1) * sub] = noise[:, q * sub : (q + 1) * sub]
    shift = shift_ref[...] * coef_ref[3]
    rows = u_ref.shape[0]
    step = 2 * strip
    for part in range(GROUP // 2):
        lanes = slice(part * step, (part + 1) * step)
        score = score_of(x_ref[:, lanes], shift, w_in_ref, w_out_ref, strip, pitch)
        inc = u_ref[:, lanes] + drift * score
        for i in range(2):
            inc_ref[2 * part + i] = inc[:, i * strip : (i + 1) * strip]
    for m in range(GROUP):
        outs[m][...] = inc_ref[lax.bitwise_xor(me, m)]
        waves[m][...] = wave_ref[lax.bitwise_xor(me, m)]


def second_kernel(
    lat, me_ref, coef_ref, anchor_ref, before_ref, after_ref, shift_ref, w_in_ref, w_out_ref, carry_ref,
    *refs,
):
    incs = refs[:GROUP]
    waves = refs[GROUP : 2 * GROUP]
    outs = refs[2 * GROUP : 3 * GROUP]
    total_ref, anc_ref, x_ref, inc_ref, wave_ref, part_ref = refs[3 * GROUP :]
    chans = anchor_ref.shape[0] // lat
    width = anchor_ref.shape[1]
    sub = width // GROUP
    pitch = sub + 2 * EDGE
    strip = lat * pitch
    me = me_ref[0]
    rows = carry_ref.shape[0]
    anc_ref[...] = jnp.zeros_like(anc_ref)
    x_ref[...] = jnp.zeros_like(x_ref)
    for l in range(lat):
        anchor = pltpu.roll(
            jnp.concatenate([anchor_ref[pl.ds(l, chans, stride=lat), :]], axis=1), lax.rem(width - me * sub, width), 1
        )
        low = jnp.where(me == 0, before_ref[0:chans, 8 * l + 6 : 8 * l + 8], anchor[:, width - 2 :])
        high = jnp.where(me == GROUP - 1, after_ref[0:chans, 8 * l + 6 : 8 * l + 8], anchor[:, sub : sub + 2])
        piece = jnp.concatenate([low, anchor[:, :sub], high], axis=1)
        anc_ref[0:chans, l * pitch + 2 : (l + 1) * pitch - 2] = piece
    for m in range(GROUP):
        inc_ref[lax.bitwise_xor(me, m)] = incs[m][...]
        wave_ref[lax.bitwise_xor(me, m)] = waves[m][...]
    state = anc_ref[...] + carry_ref[...]
    for j in range(GROUP):
        x_ref[0:rows, j * strip : (j + 1) * strip] = state
        if j + 1 < GROUP:
            state = state + inc_ref[j]
    step = 2 * strip
    for part in range(GROUP // 2):
        lanes = slice(part * step, (part + 1) * step)
        base = coef_ref.shape[0] // GROUP
        shift = jnp.concatenate(
            [
                jnp.broadcast_to(shift_ref[...] * coef_ref[(2 * part + i) * base + 3], (shift_ref.shape[0], strip))
                for i in range(2)
            ],
            axis=1,
        )
        x = x_ref[:, lanes]
        score = score_of(x, shift, w_in_ref, w_out_ref, strip, pitch)
        for i in range(2):
            level = 2 * part + i
            mine = slice(i * strip, (i + 1) * strip)
            part_ref[level] = x[0:rows, mine] * coef_ref[level * base] + score[:, mine] * coef_ref[level * base + 1]
    def compact(block):
        return jnp.concatenate([block[:, l * pitch + EDGE : l * pitch + EDGE + sub] for l in range(lat)], axis=1)

    start = compact(anc_ref[...])
    running = jnp.zeros_like(start)
    for j in range(GROUP):
        running = running + (compact(part_ref[j]) + wave_ref[j])
        wave_ref[j] = start + running
    total_ref[...] = running
    for m in range(GROUP):
        outs[m][...] = wave_ref[lax.bitwise_xor(me, m)]


def last_kernel(lat, me_ref, *refs):
    parts = refs[:GROUP]
    out_ref, all_ref = refs[GROUP:]
    chans = out_ref.shape[0] // lat
    sub = out_ref.shape[1] // GROUP
    me = me_ref[0]
    for m in range(GROUP):
        all_ref[lax.bitwise_xor(me, m)] = parts[m][...]
    for l in range(lat):
        line = jnp.concatenate([all_ref[q, 0:chans, l * sub : (l + 1) * sub] for q in range(GROUP)], axis=1)
        out_ref[pl.ds(l, chans, stride=lat), :] = line


def exchange(pieces):
    count = lax.axis_size("lvl")
    got = [pieces[0]]
    for m in range(1, GROUP):
        got.append(lax.ppermute(pieces[m], "lvl", [(k, k ^ m) for k in range(count)]))
    return got


def carried(total, block):
    count = lax.axis_size("lvl")
    blocks = count // GROUP
    carry = jnp.zeros_like(total)
    for s in range(1, blocks):
        moved = lax.ppermute(total, "lvl", [(k, (k + s * GROUP) % count) for k in range(count)])
        carry = carry + jnp.where(block >= s, moved, 0.0)
    return carry


def body(window, anchor, noise, conv_in, conv_out, time_shift, plan, start):
    _, lat, chans, width = window.shape
    hid = conv_in.shape[2]
    level = lax.axis_index("lvl")
    me = lax.rem(level, GROUP)
    block = level // GROUP
    sub = width // GROUP
    pitch = sub + 2 * EDGE
    strip = lat * pitch
    rows = up_to(chans, ROWS)
    deep = up_to(chans, PACK)

    offset = start[0] + block * GROUP
    times = lax.dynamic_slice(plan, (offset,), (GROUP + 1,)).astype(F32)
    t_now = times[:-1]
    beta = 0.1 + 19.9 * t_now / 1000.0
    step = (t_now - times[1:]) / 1000.0
    coefs = jnp.stack([0.5 * beta * step, beta * step, jnp.sqrt(beta * step), t_now / 1000.0], axis=1)
    mine = lax.dynamic_slice(coefs, (me, 0), (1, 4)).reshape(-1)
    coefs = coefs.reshape(-1)
    me_arr = me.astype(jnp.int32).reshape(1)

    def native(x):
        return jnp.transpose(x.reshape(lat, chans, width), (1, 0, 2)).reshape(chans * lat, width)

    win = native(window)
    noi = native(noise)
    anc = native(anchor)
    w_in = jnp.pad(jnp.transpose(conv_in, (1, 2, 0, 3)), ((0, 0), (0, 0), (0, 0), (0, deep - chans)))
    w_in = w_in.reshape(3 * hid, 3 * deep)
    w_out = jnp.pad(conv_out, ((0, 0), (0, 0), (0, rows - chans), (0, 0))).reshape(9 * rows, hid)
    column = time_shift.reshape(hid, 1)

    edge = (rows, 8 * lat)
    first, last = call(functools.partial(edges_kernel, lat), [edge, edge], [VM] * 3, [], 1 << 20)(win, noi, anc)
    count = lax.axis_size("lon")
    before = lax.ppermute(last, "lon", [(k, (k + 1) % count) for k in range(count)])
    after = lax.ppermute(first, "lon", [((k + 1) % count, k) for k in range(count)])

    wide = (rows, strip)
    tight = (rows, lat * sub)
    flops = 2 * 9 * chans * hid * 2 * lat * width
    made = call(
        functools.partial(first_kernel, lat),
        [wide] * GROUP + [tight] * GROUP,
        [SM, SM] + [VM] * 7,
        [
            pltpu.VMEM((deep, GROUP * strip), F32),
            pltpu.VMEM((rows, GROUP * strip), F32),
            pltpu.VMEM((GROUP,) + wide, F32),
            pltpu.VMEM((GROUP,) + tight, F32),
        ],
        flops,
    )(me_arr, mine, win, noi, before, after, column, w_in, w_out)
    incs = exchange(made[:GROUP])
    total = incs[0] + incs[1] + incs[2] + incs[3]
    carry = carried(total, block)
    waves = exchange(made[GROUP:])
    done = call(
        functools.partial(second_kernel, lat),
        [tight] * (GROUP + 1),
        [SM, SM] + [VM] * (7 + 2 * GROUP),
        [
            pltpu.VMEM(wide, F32),
            pltpu.VMEM((deep, GROUP * strip), F32),
            pltpu.VMEM((GROUP,) + wide, F32),
            pltpu.VMEM((GROUP,) + tight, F32),
            pltpu.VMEM((GROUP,) + wide, F32),
        ],
        flops,
    )(me_arr, coefs, anc, before, after, column, w_in, w_out, carry, *incs, *waves)
    carry = carried(done[GROUP], block)
    parts = exchange([part + carry for part in done[:GROUP]])
    (out,) = call(
        functools.partial(last_kernel, lat),
        [(chans * lat, width)],
        [SM] + [VM] * GROUP,
        [pltpu.VMEM((GROUP,) + tight, F32)],
        1 << 20,
    )(me_arr, *parts)
    return jnp.transpose(out.reshape(chans, lat, width), (1, 0, 2))[None]


def solution(mesh):
    return jax.shard_map(
        body,
        mesh=mesh,
        in_specs=(
            P("lvl", None, None, "lon"),
            P(None, None, "lon"),
            P("lvl", None, None, "lon"),
            P(),
            P(),
            P(),
            P(),
            P(),
        ),
        out_specs=P("lvl", None, None, "lon"),
        check_vma=False,
    )
```

```python
import functools

import jax
import jax.numpy as jnp
from jax import lax
from jax.experimental import pallas as pl
from jax.experimental.pallas import tpu as pltpu
from jax.sharding import PartitionSpec as P


GROUP = 4
EDGE = 4
ROWS = 8
PACK = 16

VM = pl.BlockSpec(memory_space=pltpu.VMEM)
SM = pl.BlockSpec(memory_space=pltpu.SMEM)
F32 = jnp.float32
BF16 = jnp.bfloat16


def up_to(value, unit):
    return -(-value // unit) * unit


def call(kernel, outs, specs, scratch, flops, limit):
    outs = [out if isinstance(out, jax.ShapeDtypeStruct) else jax.ShapeDtypeStruct(out, F32) for out in outs]
    return pl.pallas_call(
        kernel,
        out_shape=outs,
        in_specs=specs,
        out_specs=[VM] * len(outs),
        scratch_shapes=scratch,
        compiler_params=pltpu.CompilerParams(vmem_limit_bytes=limit << 20),
        cost_estimate=pl.CostEstimate(flops=flops, bytes_accessed=4 << 20, transcendentals=0),
    )


def weights_kernel(conv_in_ref, conv_out_ref, time_ref, w_in_ref, w_out_ref, column_ref, in_ref, out_ref):
    chans, hid = conv_in_ref.shape[2:]
    deep = in_ref.shape[0] // 3
    rows = out_ref.shape[0] // 9
    in_ref[...] = jnp.zeros_like(in_ref)
    out_ref[...] = jnp.zeros_like(out_ref)
    for b in range(3):
        for a in range(3):
            in_ref[a * deep : a * deep + chans, :] = conv_in_ref[a, b].astype(F32)
            tap = 3 * a + b
            out_ref[tap * rows : tap * rows + chans, :] = conv_out_ref[a, b].astype(F32)
        w_in_ref[b * hid : (b + 1) * hid, :] = jnp.transpose(in_ref[...]).astype(BF16)
    w_out_ref[...] = out_ref[...].astype(BF16)
    column_ref[...] = jnp.transpose(jnp.broadcast_to(time_ref[...], (ROWS, hid)))[:, :1]


def coefs_of(plan_ref, entry):
    now = plan_ref[entry].astype(F32)
    later = plan_ref[entry + 1].astype(F32)
    beta = 0.1 + 19.9 * now / 1000.0
    step = (now - later) / 1000.0
    spread = jnp.sqrt(jnp.full((1, 1), beta * step, F32))
    return 0.5 * beta * step, beta * step, spread, now / 1000.0


def edges_kernel(lat, win_ref, noise_ref, anchor_ref, first_ref, last_ref):
    chans = win_ref.shape[0] // lat
    width = win_ref.shape[1]
    firsts = []
    lasts = []
    for l in range(lat):
        rows = pl.ds(l, chans, stride=lat)
        win = win_ref[rows, :]
        noise = noise_ref[rows, :]
        anchor = anchor_ref[rows, :]
        firsts += [win[:, :4], noise[:, :2], anchor[:, :2]]
        lasts += [win[:, width - 4 :], noise[:, width - 2 :], anchor[:, width - 2 :]]
    first_ref[0:chans, :] = jnp.concatenate(firsts, axis=1)
    last_ref[0:chans, :] = jnp.concatenate(lasts, axis=1)


def lat_shifted(x, strip, pitch):
    size = x.shape[1]
    lane = lax.rem(lax.broadcasted_iota(jnp.int32, x.shape, 1), strip)
    below = jnp.where(lane < pitch, 0.0, pltpu.roll(x, pitch, 1))
    above = jnp.where(lane >= strip - pitch, 0.0, pltpu.roll(x, size - pitch, 1))
    return below, above


def score_of(x, shift, w_in_ref, w_out_ref, strip, pitch):
    size = x.shape[1]
    hid = w_in_ref.shape[0] // 3
    rows = w_out_ref.shape[0] // 9
    below, above = lat_shifted(x, strip, pitch)
    stacked = jnp.concatenate([below, x, above], axis=0).astype(BF16)
    taps = jnp.dot(w_in_ref[...], stacked, preferred_element_type=F32)
    pre = taps[hid : 2 * hid] + pltpu.roll(taps[:hid], 1, 1) + pltpu.roll(taps[2 * hid :], size - 1, 1)
    value = pre + shift
    hidden = (value / (1.0 + jnp.exp(-value))).astype(BF16)
    out = jnp.dot(w_out_ref[...], hidden, preferred_element_type=F32)
    lines = []
    for a in range(3):
        left = out[(3 * a) * rows : (3 * a + 1) * rows]
        mid = out[(3 * a + 1) * rows : (3 * a + 2) * rows]
        right = out[(3 * a + 2) * rows : (3 * a + 3) * rows]
        lines.append(mid + pltpu.roll(left, 1, 1) + pltpu.roll(right, size - 1, 1))
    below, _ = lat_shifted(lines[0], strip, pitch)
    _, above = lat_shifted(lines[2], strip, pitch)
    return lines[1] + below + above


def first_kernel(
    lat, where_ref, plan_ref, win_ref, noise_ref, before_ref, after_ref, shift_ref, w_in_ref, w_out_ref,
    *refs,
):
    outs = refs[:GROUP]
    waves = refs[GROUP : 2 * GROUP]
    x_ref, u_ref, inc_ref, wave_ref = refs[2 * GROUP :]
    chans = win_ref.shape[0] // lat
    width = win_ref.shape[1]
    sub = width // GROUP
    pitch = sub + 2 * EDGE
    strip = lat * pitch
    me = where_ref[0]
    half, drift, spread, time = coefs_of(plan_ref, where_ref[1] + me)
    x_ref[...] = jnp.zeros_like(x_ref)
    u_ref[...] = jnp.zeros_like(u_ref)
    blank = jnp.zeros((chans, 2), F32)
    for l in range(lat):
        rows = pl.ds(l, chans, stride=lat)
        win = win_ref[rows, :]
        noise = noise_ref[rows, :] * spread
        low = before_ref[0:chans, 8 * l : 8 * l + 8]
        high = after_ref[0:chans, 8 * l : 8 * l + 8]
        wide = jnp.concatenate([low[:, :4], win, high[:, :4]], axis=1)
        other = jnp.concatenate([blank, low[:, 4:6] * spread, noise, high[:, 4:6] * spread, blank], axis=1)
        total = wide * half + other
        for q in range(GROUP):
            lanes = slice(q * strip + l * pitch, q * strip + (l + 1) * pitch)
            x_ref[0:chans, lanes] = wide[:, q * sub : q * sub + pitch]
            u_ref[0:chans, lanes] = total[:, q * sub : q * sub + pitch]
            wave_ref[q, 0:chans, l * sub : (l + 1) * sub] = noise[:, q * sub : (q + 1) * sub]
    shift = shift_ref[...] * time
    step = 2 * strip
    for part in range(GROUP // 2):
        lanes = slice(part * step, (part + 1) * step)
        score = score_of(x_ref[:, lanes], shift, w_in_ref, w_out_ref, strip, pitch)
        inc = u_ref[:, lanes] + drift * score
        for i in range(2):
            inc_ref[2 * part + i] = inc[:, i * strip : (i + 1) * strip]
    for m in range(GROUP):
        outs[m][...] = inc_ref[lax.bitwise_xor(me, m)]
        waves[m][...] = wave_ref[lax.bitwise_xor(me, m)]


def second_kernel(
    lat, where_ref, plan_ref, anchor_ref, before_ref, after_ref, shift_ref, w_in_ref, w_out_ref, carry_ref,
    *refs,
):
    incs = refs[:GROUP]
    waves = refs[GROUP : 2 * GROUP]
    outs = refs[2 * GROUP : 3 * GROUP]
    total_ref, anc_ref, x_ref, inc_ref, wave_ref, part_ref = refs[3 * GROUP :]
    chans = anchor_ref.shape[0] // lat
    width = anchor_ref.shape[1]
    sub = width // GROUP
    pitch = sub + 2 * EDGE
    strip = lat * pitch
    me = where_ref[0]
    coefs = [coefs_of(plan_ref, where_ref[1] + j) for j in range(GROUP)]
    rows = carry_ref.shape[0]
    anc_ref[...] = jnp.zeros_like(anc_ref)
    x_ref[...] = jnp.zeros_like(x_ref)
    for l in range(lat):
        anchor = pltpu.roll(
            jnp.concatenate([anchor_ref[pl.ds(l, chans, stride=lat), :]], axis=1), lax.rem(width - me * sub, width), 1
        )
        low = jnp.where(me == 0, before_ref[0:chans, 8 * l + 6 : 8 * l + 8], anchor[:, width - 2 :])
        high = jnp.where(me == GROUP - 1, after_ref[0:chans, 8 * l + 6 : 8 * l + 8], anchor[:, sub : sub + 2])
        piece = jnp.concatenate([low, anchor[:, :sub], high], axis=1)
        anc_ref[0:chans, l * pitch + 2 : (l + 1) * pitch - 2] = piece
    for m in range(GROUP):
        inc_ref[lax.bitwise_xor(me, m)] = incs[m][...]
        wave_ref[lax.bitwise_xor(me, m)] = waves[m][...]
    state = anc_ref[...] + carry_ref[...]
    for j in range(GROUP):
        x_ref[0:rows, j * strip : (j + 1) * strip] = state
        if j + 1 < GROUP:
            state = state + inc_ref[j]
    step = 2 * strip
    for part in range(GROUP // 2):
        lanes = slice(part * step, (part + 1) * step)
        shift = jnp.concatenate(
            [
                jnp.broadcast_to(shift_ref[...] * coefs[2 * part + i][3], (shift_ref.shape[0], strip))
                for i in range(2)
            ],
            axis=1,
        )
        x = x_ref[:, lanes]
        score = score_of(x, shift, w_in_ref, w_out_ref, strip, pitch)
        for i in range(2):
            level = 2 * part + i
            mine = slice(i * strip, (i + 1) * strip)
            part_ref[level] = x[0:rows, mine] * coefs[level][0] + score[:, mine] * coefs[level][1]

    def compact(block):
        return jnp.concatenate([block[:, l * pitch + EDGE : l * pitch + EDGE + sub] for l in range(lat)], axis=1)

    start = compact(anc_ref[...])
    running = jnp.zeros_like(start)
    for j in range(GROUP):
        running = running + (compact(part_ref[j]) + wave_ref[j])
        wave_ref[j] = start + running
    total_ref[...] = running
    for m in range(GROUP):
        outs[m][...] = wave_ref[lax.bitwise_xor(me, m)]


def last_kernel(lat, where_ref, *refs):
    parts = refs[:GROUP]
    out_ref, all_ref = refs[GROUP:]
    chans = out_ref.shape[0] // lat
    sub = out_ref.shape[1] // GROUP
    me = where_ref[0]
    for m in range(GROUP):
        all_ref[lax.bitwise_xor(me, m)] = parts[m][...]
    for l in range(lat):
        line = jnp.concatenate([all_ref[q, 0:chans, l * sub : (l + 1) * sub] for q in range(GROUP)], axis=1)
        out_ref[pl.ds(l, chans, stride=lat), :] = line


def exchange(pieces):
    count = lax.axis_size("lvl")
    got = [pieces[0]]
    for m in range(1, GROUP):
        got.append(lax.ppermute(pieces[m], "lvl", [(k, k ^ m) for k in range(count)]))
    return got


def carried(total, block):
    count = lax.axis_size("lvl")
    blocks = count // GROUP
    carry = jnp.zeros_like(total)
    for s in range(1, blocks):
        moved = lax.ppermute(total, "lvl", [(k, (k + s * GROUP) % count) for k in range(count)])
        carry = carry + jnp.where(block >= s, moved, 0.0)
    return carry


def body(window, anchor, noise, conv_in, conv_out, time_shift, plan, start):
    _, lat, chans, width = window.shape
    hid = conv_in.shape[2]
    level = lax.axis_index("lvl")
    me = lax.rem(level, GROUP)
    block = level // GROUP
    sub = width // GROUP
    pitch = sub + 2 * EDGE
    strip = lat * pitch
    rows = up_to(chans, ROWS)
    deep = up_to(chans, PACK)

    where = jnp.stack([me, start[0] + block * GROUP]).astype(jnp.int32)

    def native(x):
        return jnp.transpose(x.reshape(lat, chans, width), (1, 0, 2)).reshape(chans * lat, width)

    win = native(window)
    noi = native(noise)
    anc = native(anchor)
    w_in, w_out, column = call(
        weights_kernel,
        [
            jax.ShapeDtypeStruct((3 * hid, 3 * deep), BF16),
            jax.ShapeDtypeStruct((9 * rows, hid), BF16),
            jax.ShapeDtypeStruct((hid, 1), F32),
        ],
        [VM] * 3,
        [pltpu.VMEM((3 * deep, hid), F32), pltpu.VMEM((9 * rows, hid), F32)],
        1 << 24,
        8,
    )(jnp.swapaxes(conv_in, 2, 3), conv_out, time_shift.reshape(1, hid))

    edge = (rows, 8 * lat)
    first, last = call(functools.partial(edges_kernel, lat), [edge, edge], [VM] * 3, [], 1 << 20, 8)(win, noi, anc)
    count = lax.axis_size("lon")
    before = lax.ppermute(last, "lon", [(k, (k + 1) % count) for k in range(count)])
    after = lax.ppermute(first, "lon", [((k + 1) % count, k) for k in range(count)])

    wide = (rows, strip)
    tight = (rows, lat * sub)
    flops = 2 * 9 * chans * hid * 2 * lat * width
    made = call(
        functools.partial(first_kernel, lat),
        [wide] * GROUP + [tight] * GROUP,
        [SM, SM] + [VM] * 7,
        [
            pltpu.VMEM((deep, GROUP * strip), F32),
            pltpu.VMEM((rows, GROUP * strip), F32),
            pltpu.VMEM((GROUP,) + wide, F32),
            pltpu.VMEM((GROUP,) + tight, F32),
        ],
        flops,
        24,
    )(where, plan, win, noi, before, after, column, w_in, w_out)
    incs = exchange(made[:GROUP])
    total = incs[0] + incs[1] + incs[2] + incs[3]
    carry = carried(total, block)
    waves = exchange(made[GROUP:])
    done = call(
        functools.partial(second_kernel, lat),
        [tight] * (GROUP + 1),
        [SM, SM] + [VM] * (7 + 2 * GROUP),
        [
            pltpu.VMEM(wide, F32),
            pltpu.VMEM((deep, GROUP * strip), F32),
            pltpu.VMEM((GROUP,) + wide, F32),
            pltpu.VMEM((GROUP,) + tight, F32),
            pltpu.VMEM((GROUP,) + wide, F32),
        ],
        flops,
        24,
    )(where, plan, anc, before, after, column, w_in, w_out, carry, *incs, *waves)
    carry = carried(done[GROUP], block)
    parts = exchange([part + carry for part in done[:GROUP]])
    (out,) = call(
        functools.partial(last_kernel, lat),
        [(chans * lat, width)],
        [SM] + [VM] * GROUP,
        [pltpu.VMEM((GROUP,) + tight, F32)],
        1 << 20,
        8,
    )(where, *parts)
    return jnp.transpose(out.reshape(chans, lat, width), (1, 0, 2))[None]


def solution(mesh):
    return jax.shard_map(
        body,
        mesh=mesh,
        in_specs=(
            P("lvl", None, None, "lon"),
            P(None, None, "lon"),
            P("lvl", None, None, "lon"),
            P(),
            P(),
            P(),
            P(),
            P(),
        ),
        out_specs=P("lvl", None, None, "lon"),
        check_vma=False,
    )
```

```python
import functools

import jax
import jax.numpy as jnp
from jax import lax
from jax.experimental import pallas as pl
from jax.experimental.pallas import tpu as pltpu
from jax.sharding import PartitionSpec as P


GROUP = 4
EDGE = 4
SLOT = 2 * EDGE
ROWS = 8
PACK = 16
COEFS = 8

VM = pl.BlockSpec(memory_space=pltpu.VMEM)
SM = pl.BlockSpec(memory_space=pltpu.SMEM)
ANY = pl.BlockSpec(memory_space=pl.ANY)
F32 = jnp.float32
BF16 = jnp.bfloat16


def up_to(value, unit):
    return -(-value // unit) * unit


def call(kernel, outs, specs, scratch, flops, limit, out_specs=None):
    outs = [out if isinstance(out, jax.ShapeDtypeStruct) else jax.ShapeDtypeStruct(out, F32) for out in outs]
    return pl.pallas_call(
        kernel,
        out_shape=outs,
        in_specs=specs,
        out_specs=out_specs or [VM] * len(outs),
        scratch_shapes=scratch,
        compiler_params=pltpu.CompilerParams(vmem_limit_bytes=limit << 20),
        cost_estimate=pl.CostEstimate(flops=flops, bytes_accessed=4 << 20, transcendentals=0),
    )


def roll(x, shift):
    shift = shift % x.shape[1]
    return pltpu.roll(x, shift, 1) if shift else x


def lanes_of(x):
    return lax.broadcasted_iota(jnp.int32, x.shape, 1)


def between(lane, low, high):
    return jnp.logical_and(lane >= low, lane < high)


def swapped(arrays):
    count = len(arrays)
    sub = arrays[0].shape[1] // count
    block = lanes_of(arrays[0]) // sub
    turned = []
    for r in range(count):
        mixed = arrays[r]
        for j in range(1, count):
            mixed = jnp.where(block == j, arrays[(j + r) % count], mixed)
        turned.append(roll(mixed, r * sub))
    outs = []
    for j in range(count):
        mixed = turned[(0 - j) % count]
        for i in range(1, count):
            mixed = jnp.where(block == i, turned[(i - j) % count], mixed)
        outs.append(mixed)
    return outs


def edges_kernel(lat, win_any, noise_any, anchor_any, first_ref, last_ref, win_ref, noise_ref, anchor_ref, sems):
    copies = [
        pltpu.make_async_copy(source, target, sems.at[i])
        for i, (source, target) in enumerate(
            [(win_any, win_ref), (noise_any, noise_ref), (anchor_any, anchor_ref)]
        )
    ]
    for copy in copies:
        copy.start()
    chans = win_ref.shape[0] // lat
    tiles = []
    for copy, ref, shift, skip in zip(copies, (win_ref, noise_ref, anchor_ref), (4, 6, 8), (0, 0, 6)):
        copy.wait()
        tile = roll(ref[pl.ds(0, chans, stride=lat), :], shift)
        width = tile.shape[1]
        slot = lax.rem(lanes_of(tile) + width - skip, width) // SLOT
        for l in range(1, lat):
            tile = jnp.where(slot == l, roll(ref[pl.ds(l, chans, stride=lat), :], SLOT * l + shift), tile)
        tiles.append(tile)
    win, noise, anchor = tiles
    spot = lax.rem(lanes_of(win), SLOT)
    last = jnp.where(spot < 4, win, jnp.where(spot < 6, noise, anchor))
    first = jnp.where(spot < 2, roll(noise, -6), jnp.where(spot < 4, roll(anchor, -6), win))
    for ref, value in ((first_ref, first), (last_ref, last)):
        ref[...] = jnp.zeros_like(ref)
        ref[0:chans, :] = value


def tiled(rolled, pitch, turn):
    lat = len(rolled)
    width = rolled[0].shape[1]
    lane = lanes_of(rolled[0])
    tiles = []
    for t in range(lat * pitch // width):
        tile = None
        for slot in range(lat):
            low = slot * pitch - t * width
            if low >= width or low + pitch <= 0:
                continue
            piece = rolled[(slot - turn) % lat]
            tile = piece if tile is None else jnp.where(lane >= low, piece, tile)
        tiles.append(tile)
    return tiles


def turn_of(pitch, sub, width):
    return next(k for k in range(width) if (pitch * k) % width == sub)


def coefs_of(plan_ref, entry):
    now = plan_ref[entry].astype(F32)
    later = plan_ref[entry + 1].astype(F32)
    beta = 0.1 + 19.9 * now / 1000.0
    step = (now - later) / 1000.0
    return [0.5 * beta * step, beta * step, jnp.sqrt(jnp.full((1, 1), beta * step, F32)), now / 1000.0]


def build_kernel(
    lat, start_ref, plan_ref, conv_in_ref, conv_out_ref, time_ref, win_ref, noise_ref,
    w_in_ref, w_out_ref, column_ref, coef_ref, x_ref, n_ref, *refs,
):
    waves = refs[:GROUP]
    in_ref, out_ref, wave_ref = refs[GROUP:]
    chans, hid = conv_in_ref.shape[2:]
    width = win_ref.shape[1]
    deep = in_ref.shape[0] // 9
    rows = n_ref.shape[1]
    in_ref[...] = jnp.zeros_like(in_ref)
    out_ref[...] = jnp.zeros_like(out_ref)
    for b in range(3):
        for a in range(3):
            tap = 3 * b + a
            in_ref[tap * deep : tap * deep + chans, :] = conv_in_ref[a, b].astype(F32)
            out_ref[a * rows : a * rows + chans, b * hid : (b + 1) * hid] = conv_out_ref[a, b].astype(F32)
    w_in_ref[...] = jnp.transpose(in_ref[...]).astype(BF16)
    w_out_ref[...] = out_ref[...].astype(BF16)
    column_ref[...] = jnp.transpose(jnp.broadcast_to(time_ref[...], (ROWS, hid)))[:, :1]

    level = lax.axis_index("lvl")
    me = lax.rem(level, GROUP)
    entries = [level] + [level - me + j for j in range(GROUP)]
    for i, entry in enumerate(entries):
        values = coefs_of(plan_ref, start_ref[0] + entry)
        for r, value in enumerate(values):
            coef_ref[COEFS * i + r : COEFS * i + r + 1, :] = jnp.broadcast_to(
                value if r == 2 else jnp.full((1, 1), value, F32), (1, coef_ref.shape[1])
            )
    sub = width // GROUP
    pitch = sub + 2 * EDGE
    turn = turn_of(pitch, sub, width)
    for source, target in ((win_ref, x_ref), (noise_ref, n_ref)):
        target[:, chans // ROWS * ROWS :, :] = jnp.zeros_like(target[:, chans // ROWS * ROWS :, :])
        rolled = [roll(source[pl.ds(l, chans, stride=lat), :], pitch * l + EDGE) for l in range(lat)]
        for q in range(GROUP):
            for t, tile in enumerate(tiled(rolled, pitch, turn * q)):
                target[q, 0:chans, t * width : (t + 1) * width] = tile
    spread = coef_ref[2:3, 0:1]
    wave_ref[:, chans // ROWS * ROWS :, :] = jnp.zeros_like(wave_ref[:, chans // ROWS * ROWS :, :])
    for t in range(lat // GROUP):
        lines = [noise_ref[pl.ds(GROUP * t + i, chans, stride=lat), :] * spread for i in range(GROUP)]
        for q, line in enumerate(swapped(lines)):
            wave_ref[q, 0:chans, t * width : (t + 1) * width] = line
    for m in range(GROUP):
        waves[m][...] = wave_ref[lax.bitwise_xor(me, m)]


def lat_shifted(x, pitch, first):
    lane = lanes_of(x)
    slots = x.shape[1] // pitch
    zero = jnp.zeros_like(x)
    final = (first - 1) % slots
    below = jnp.where(between(lane, first * pitch, (first + 1) * pitch), zero, roll(x, pitch))
    above = jnp.where(between(lane, final * pitch, (final + 1) * pitch), zero, roll(x, -pitch))
    return below, above


def scores_of(strips, shifts, firsts, w_in_ref, w_out_ref, pitch):
    strip = strips[0].shape[1]
    rows = w_out_ref.shape[0] // 3
    stacks = []
    for x, first in zip(strips, firsts):
        x = x.astype(BF16)
        stack = []
        for moved in (roll(x, 1), x, roll(x, -1)):
            below, above = lat_shifted(moved, pitch, first)
            stack += [below, moved, above]
        stacks.append(jnp.concatenate(stack, axis=0))
    pre = jnp.dot(w_in_ref[...], jnp.concatenate(stacks, axis=1), preferred_element_type=F32)
    hiddens = []
    for i, shift in enumerate(shifts):
        value = pre[:, i * strip : (i + 1) * strip] + shift
        hidden = (value / (1.0 + jnp.exp(-value))).astype(BF16)
        hiddens.append(jnp.concatenate([roll(hidden, 1), hidden, roll(hidden, -1)], axis=0))
    out = jnp.dot(w_out_ref[...], jnp.concatenate(hiddens, axis=1), preferred_element_type=F32)
    scores = []
    for i, first in enumerate(firsts):
        lines = out[:, i * strip : (i + 1) * strip]
        below, _ = lat_shifted(lines[:rows], pitch, first)
        _, above = lat_shifted(lines[2 * rows :], pitch, first)
        scores.append(lines[rows : 2 * rows] + below + above)
    return scores


def edged(strip, edges, pitch, turn, source, target, count, chosen=None):
    width = edges.shape[1]
    lat = strip.shape[1] // pitch
    lane = lanes_of(strip)
    moves = {}
    for l in range(lat):
        slot = (l + turn) % lat
        moves.setdefault((slot * pitch + target - SLOT * l - source) % width, []).append(slot)
    for shift, slots in moves.items():
        moved = jnp.concatenate([roll(edges, shift)] * (strip.shape[1] // width), axis=1)
        mask = None
        for slot in slots:
            here = between(lane, slot * pitch + target, slot * pitch + target + count)
            mask = here if mask is None else jnp.logical_or(mask, here)
        if chosen is not None:
            mask = jnp.logical_and(mask, chosen)
        strip = jnp.where(mask, moved, strip)
    return strip


def first_kernel(lat, coef_ref, x_ref, n_ref, before_ref, after_ref, column_ref, w_in_ref, w_out_ref, *refs):
    outs = refs[:GROUP]
    (inc_ref,) = refs[GROUP:]
    rows = n_ref.shape[1]
    strip = n_ref.shape[2]
    width = before_ref.shape[1]
    sub = width // GROUP
    pitch = strip // lat
    turn = turn_of(pitch, sub, width)
    me = lax.rem(lax.axis_index("lvl"), GROUP)
    half, drift, spread, time = [coef_ref[r : r + 1, 0:1] for r in range(4)]
    shift = column_ref[...] * time
    before = before_ref[...]
    after = after_ref[...]
    tail = x_ref.shape[1] - rows
    for part in range(GROUP // 2):
        quarters = (2 * part, 2 * part + 1)
        strips = []
        others = []
        for q in quarters:
            x = x_ref[q, 0:rows]
            noise = n_ref[q]
            if q == 0:
                x = edged(x, before, pitch, turn * q, 0, 0, 4)
                noise = edged(noise, before, pitch, turn * q, 4, 2, 2)
            if q == GROUP - 1:
                x = edged(x, after, pitch, turn * q, 4, pitch - EDGE, 4)
                noise = edged(noise, after, pitch, turn * q, 0, pitch - EDGE, 2)
            strips.append(jnp.concatenate([x, jnp.zeros((tail, strip), F32)], axis=0))
            others.append(x * half + noise * spread)
        firsts = [(turn * q) % lat for q in quarters]
        scores = scores_of(strips, [shift, shift], firsts, w_in_ref, w_out_ref, pitch)
        for q, score, other in zip(quarters, scores, others):
            inc_ref[q] = roll(other + drift * score, -pitch * turn * q)
    for m in range(GROUP):
        outs[m][...] = inc_ref[lax.bitwise_xor(me, m)]


def base_kernel(lat, anchor_ref, before_ref, after_ref, *refs):
    incs = refs[:GROUP]
    base_ref, tight_ref, inc_ref, anc_ref = refs[GROUP:]
    chans = anchor_ref.shape[0] // lat
    width = anchor_ref.shape[1]
    sub = width // GROUP
    strip = base_ref.shape[2]
    pitch = strip // lat
    me = lax.rem(lax.axis_index("lvl"), GROUP)
    for m in range(GROUP):
        inc_ref[lax.bitwise_xor(me, m)] = incs[m][...]
    anc_ref[chans // ROWS * ROWS :, :] = jnp.zeros_like(anc_ref[chans // ROWS * ROWS :, :])
    tight_ref[chans // ROWS * ROWS :, :] = jnp.zeros_like(tight_ref[chans // ROWS * ROWS :, :])
    turned = []
    for l in range(lat):
        turned.append(pltpu.roll(anchor_ref[pl.ds(l, chans, stride=lat), :], lax.rem(width - me * sub, width), 1))
    for t, tile in enumerate(tiled([roll(line, pitch * l + EDGE) for l, line in enumerate(turned)], pitch, 0)):
        anc_ref[0:chans, t * width : (t + 1) * width] = tile
    block = lanes_of(turned[0]) // sub
    for t in range(lat // GROUP):
        tile = turned[GROUP * t]
        for i in range(1, GROUP):
            tile = jnp.where(block == i, roll(turned[GROUP * t + i], i * sub), tile)
        tight_ref[0:chans, t * width : (t + 1) * width] = tile
    state = edged(anc_ref[...], before_ref[...], pitch, 0, 6, 2, 2, me == 0)
    state = edged(state, after_ref[...], pitch, 0, 2, pitch - EDGE, 2, me == GROUP - 1)
    for j in range(GROUP):
        base_ref[j] = state
        if j + 1 < GROUP:
            state = state + inc_ref[j]


def second_kernel(
    lat, coef_ref, base_ref, tight_ref, column_ref, w_in_ref, w_out_ref, carry_ref, *refs,
):
    waves = refs[:GROUP]
    outs = refs[GROUP : 2 * GROUP]
    total_ref, wave_ref = refs[2 * GROUP :]
    rows, strip = carry_ref.shape
    pitch = strip // lat
    width = coef_ref.shape[1]
    sub = width // GROUP
    me = lax.rem(lax.axis_index("lvl"), GROUP)
    for m in range(GROUP):
        wave_ref[lax.bitwise_xor(me, m)] = waves[m][...]
    tail = w_in_ref.shape[1] // 9 - rows
    carry = carry_ref[...]

    def packed(block):
        tiles = [block[:, t * width : (t + 1) * width] for t in range(strip // width)]
        lane = lanes_of(tiles[0])
        outs = []
        for l in range(lat):
            low = l * pitch + EDGE
            piece = tiles[low // width]
            if (low + sub - 1) // width != low // width:
                piece = jnp.where(lane >= low % width, piece, tiles[low // width + 1])
            moved = roll(piece, (l % GROUP) * sub - low)
            outs.append(moved if l % GROUP == 0 else jnp.where(lane >= (l % GROUP) * sub, moved, outs.pop()))
        return jnp.concatenate(outs, axis=1)

    running = jnp.zeros_like(total_ref)
    for part in range(GROUP // 2):
        levels = (2 * part, 2 * part + 1)
        states = [base_ref[j] + carry for j in levels]
        strips = [jnp.concatenate([x, jnp.zeros((tail, strip), F32)], axis=0) for x in states]
        coefs = [[coef_ref[COEFS * (j + 1) + r : COEFS * (j + 1) + r + 1, 0:1] for r in range(4)] for j in levels]
        shifts = [column_ref[...] * coef[3] for coef in coefs]
        scores = scores_of(strips, shifts, [0, 0], w_in_ref, w_out_ref, pitch)
        for j, x, score, coef in zip(levels, states, scores, coefs):
            running = running + (packed(x * coef[0] + score * coef[1]) + wave_ref[j])
            wave_ref[j] = tight_ref[...] + running
    total_ref[...] = running
    for m in range(GROUP):
        outs[m][...] = wave_ref[lax.bitwise_xor(me, m)]


def last_kernel(lat, *refs):
    parts = refs[:GROUP]
    out_any, all_ref, line_ref, sems = refs[GROUP:]
    chans = line_ref.shape[0] // lat
    width = line_ref.shape[1]
    me = lax.rem(lax.axis_index("lvl"), GROUP)
    for m in range(GROUP):
        all_ref[lax.bitwise_xor(me, m)] = parts[m][...]
    size = up_to(-(-chans // 3), ROWS)
    copies = []
    for i, low in enumerate(range(0, chans, size)):
        high = min(low + size, chans)
        for t in range(lat // GROUP):
            lanes = slice(t * width, (t + 1) * width)
            lines = swapped([all_ref[q, low:high, lanes] for q in range(GROUP)])
            for k, line in enumerate(lines):
                line_ref[pl.ds(low * lat + GROUP * t + k, high - low, stride=lat), :] = line
        spot = pl.ds(low * lat, (high - low) * lat)
        copies.append(pltpu.make_async_copy(line_ref.at[spot], out_any.at[spot], sems.at[i]))
        copies[-1].start()
    for copy in copies:
        copy.wait()


def exchange(pieces):
    count = lax.axis_size("lvl")
    got = [pieces[0]]
    for m in range(1, GROUP):
        got.append(lax.ppermute(pieces[m], "lvl", [(k, k ^ m) for k in range(count)]))
    return got


def carried(total, block):
    count = lax.axis_size("lvl")
    blocks = count // GROUP
    carry = jnp.zeros_like(total)
    for s in range(1, blocks):
        moved = lax.ppermute(total, "lvl", [(k, (k + s * GROUP) % count) for k in range(count)])
        carry = carry + jnp.where(block >= s, moved, 0.0)
    return carry


def body(window, anchor, noise, conv_in, conv_out, time_shift, plan, start):
    _, lat, chans, width = window.shape
    hid = conv_in.shape[2]
    block = lax.axis_index("lvl") // GROUP
    sub = width // GROUP
    strip = lat * (sub + 2 * EDGE)
    rows = up_to(chans, ROWS)
    deep = up_to(chans, PACK)

    def native(x):
        return jnp.transpose(x.reshape(lat, chans, width), (1, 0, 2)).reshape(chans * lat, width)

    win = native(window)
    noi = native(noise)
    anc = native(anchor)
    edge = (rows, SLOT * lat)
    wide = (rows, strip)
    tight = (rows, lat * sub)
    flops = 2 * 9 * chans * hid * 2 * lat * width
    whole = pltpu.VMEM((chans * lat, width), F32)

    first, last = call(
        functools.partial(edges_kernel, lat),
        [edge, edge],
        [ANY] * 3,
        [whole] * 3 + [pltpu.SemaphoreType.DMA((3,))],
        1 << 20,
        8,
    )(win, noi, anc)
    count = lax.axis_size("lon")
    before = lax.ppermute(last, "lon", [(k, (k + 1) % count) for k in range(count)])
    after = lax.ppermute(first, "lon", [((k + 1) % count, k) for k in range(count)])
    w_in, w_out, column, coefs, x, n, *waves = call(
        functools.partial(build_kernel, lat),
        [
            jax.ShapeDtypeStruct((hid, 9 * deep), BF16),
            jax.ShapeDtypeStruct((3 * rows, 3 * hid), BF16),
            jax.ShapeDtypeStruct((hid, 1), F32),
            (COEFS * (GROUP + 1), width),
            (GROUP, deep, strip),
            (GROUP,) + wide,
        ]
        + [tight] * GROUP,
        [SM, SM] + [VM] * 5,
        [pltpu.VMEM((9 * deep, hid), F32), pltpu.VMEM((3 * rows, 3 * hid), F32), pltpu.VMEM((GROUP,) + tight, F32)],
        flops // 4,
        12,
    )(start, plan, jnp.swapaxes(conv_in, 2, 3), conv_out, time_shift.reshape(1, hid), win, noi)
    incs = call(
        functools.partial(first_kernel, lat),
        [wide] * GROUP,
        [VM] * 8,
        [pltpu.VMEM((GROUP,) + wide, F32)],
        flops,
        20,
    )(coefs, x, n, before, after, column, w_in, w_out)
    incs = exchange(incs)
    total = incs[0] + incs[1] + incs[2] + incs[3]
    carry = carried(total, block)
    waves = exchange(waves)
    base, packed = call(
        functools.partial(base_kernel, lat),
        [(GROUP,) + wide, tight],
        [VM] * (3 + GROUP),
        [pltpu.VMEM((GROUP,) + wide, F32), pltpu.VMEM(wide, F32)],
        flops // 4,
        12,
    )(anc, before, after, *incs)
    done = call(
        functools.partial(second_kernel, lat),
        [tight] * (GROUP + 1),
        [VM] * (7 + GROUP),
        [pltpu.VMEM((GROUP,) + tight, F32)],
        flops,
        20,
    )(coefs, base, packed, column, w_in, w_out, carry, *waves)
    carry = carried(done[GROUP], block)
    parts = exchange([part + carry for part in done[:GROUP]])
    (out,) = call(
        functools.partial(last_kernel, lat),
        [(chans * lat, width)],
        [VM] * GROUP,
        [pltpu.VMEM((GROUP,) + tight, F32), whole, pltpu.SemaphoreType.DMA((3,))],
        1 << 20,
        8,
        [ANY],
    )(*parts)
    return jnp.transpose(out.reshape(chans, lat, width), (1, 0, 2))[None]


def solution(mesh):
    return jax.shard_map(
        body,
        mesh=mesh,
        in_specs=(
            P("lvl", None, None, "lon"),
            P(None, None, "lon"),
            P("lvl", None, None, "lon"),
            P(),
            P(),
            P(),
            P(),
            P(),
        ),
        out_specs=P("lvl", None, None, "lon"),
        check_vma=False,
    )
```

```python
import functools

import jax
import jax.numpy as jnp
from jax import lax
from jax.experimental import pallas as pl
from jax.experimental.pallas import tpu as pltpu
from jax.sharding import PartitionSpec as P


GROUP = 4
EDGE = 4
SLOT = 2 * EDGE
ROWS = 8
PACK = 16
COEFS = 8

VM = pl.BlockSpec(memory_space=pltpu.VMEM)
SM = pl.BlockSpec(memory_space=pltpu.SMEM)
HBM = pl.BlockSpec(memory_space=pltpu.HBM)
F32 = jnp.float32
BF16 = jnp.bfloat16


def up_to(value, unit):
    return -(-value // unit) * unit


def call(kernel, outs, specs, scratch, flops, limit, out_specs=None):
    outs = [out if isinstance(out, jax.ShapeDtypeStruct) else jax.ShapeDtypeStruct(out, F32) for out in outs]
    return pl.pallas_call(
        kernel,
        out_shape=outs,
        in_specs=specs,
        out_specs=out_specs or [VM] * len(outs),
        scratch_shapes=scratch,
        compiler_params=pltpu.CompilerParams(vmem_limit_bytes=int(limit * (1 << 20))),
        cost_estimate=pl.CostEstimate(flops=flops, bytes_accessed=4 << 20, transcendentals=0),
    )


def roll(x, shift):
    shift = shift % x.shape[1]
    return pltpu.roll(x, shift, 1) if shift else x


def lanes_of(x):
    return lax.broadcasted_iota(jnp.int32, x.shape, 1)


def between(lane, low, high):
    return jnp.logical_and(lane >= low, lane < high)


def swapped(arrays):
    count = len(arrays)
    sub = arrays[0].shape[1] // count
    block = lanes_of(arrays[0]) // sub
    turned = []
    for r in range(count):
        mixed = arrays[r]
        for j in range(1, count):
            mixed = jnp.where(block == j, arrays[(j + r) % count], mixed)
        turned.append(roll(mixed, r * sub))
    outs = []
    for j in range(count):
        mixed = turned[(0 - j) % count]
        for i in range(1, count):
            mixed = jnp.where(block == i, turned[(i - j) % count], mixed)
        outs.append(mixed)
    return outs


def coefs_of(plan_ref, entry):
    now = plan_ref[entry].astype(F32)
    later = plan_ref[entry + 1].astype(F32)
    beta = 0.1 + 19.9 * now / 1000.0
    step = (now - later) / 1000.0
    return [0.5 * beta * step, beta * step, jnp.sqrt(jnp.full((1, 1), beta * step, F32)), now / 1000.0]


def edges_kernel(
    lat, start_ref, plan_hbm, win_hbm, noise_hbm, anchor_hbm, conv_in_hbm, conv_out_hbm, time_hbm,
    first_ref, last_ref, coef_ref, win_ref, noise_ref, anchor_ref, conv_in_ref, conv_out_ref, time_ref,
    plan_ref, sems,
):
    pairs = [
        (plan_hbm, plan_ref),
        (win_hbm, win_ref),
        (noise_hbm, noise_ref),
        (anchor_hbm, anchor_ref),
        (conv_in_hbm, conv_in_ref),
        (conv_out_hbm, conv_out_ref),
        (time_hbm, time_ref),
    ]
    copies = [pltpu.make_async_copy(source, target, sems.at[i]) for i, (source, target) in enumerate(pairs)]
    for copy in copies:
        copy.start()
    copies[0].wait()
    copies = copies[1:]
    level = lax.axis_index("lvl")
    entries = [level] + [level - lax.rem(level, GROUP) + j for j in range(GROUP)]
    for i, entry in enumerate(entries):
        values = coefs_of(plan_ref, start_ref[0] + entry)
        for r, value in enumerate(values):
            coef_ref[COEFS * i + r : COEFS * i + r + 1, :] = jnp.broadcast_to(
                value if r == 2 else jnp.full((1, 1), value, F32), (1, coef_ref.shape[1])
            )
    chans = win_ref.shape[0] // lat
    tiles = []
    for copy, ref, shift, skip in zip(copies, (win_ref, noise_ref, anchor_ref), (4, 6, 8), (0, 0, 6)):
        copy.wait()
        tile = roll(ref[pl.ds(0, chans, stride=lat), :], shift)
        width = tile.shape[1]
        slot = lax.rem(lanes_of(tile) + width - skip, width) // SLOT
        for l in range(1, lat):
            tile = jnp.where(slot == l, roll(ref[pl.ds(l, chans, stride=lat), :], SLOT * l + shift), tile)
        tiles.append(tile)
    win, noise, anchor = tiles
    spot = lax.rem(lanes_of(win), SLOT)
    last = jnp.where(spot < 4, win, jnp.where(spot < 6, noise, anchor))
    first = jnp.where(spot < 2, roll(noise, -6), jnp.where(spot < 4, roll(anchor, -6), win))
    for ref, value in ((first_ref, first), (last_ref, last)):
        ref[...] = jnp.zeros_like(ref)
        ref[0:chans, :] = value
    for copy in copies[3:]:
        copy.wait()


def tiled(rolled, pitch, turn):
    lat = len(rolled)
    width = rolled[0].shape[1]
    lane = lanes_of(rolled[0])
    tiles = []
    for t in range(lat * pitch // width):
        tile = None
        for slot in range(lat):
            low = slot * pitch - t * width
            if low >= width or low + pitch <= 0:
                continue
            piece = rolled[(slot - turn) % lat]
            tile = piece if tile is None else jnp.where(lane >= low, piece, tile)
        tiles.append(tile)
    return tiles


def turn_of(pitch, sub, width):
    return next(k for k in range(width) if (pitch * k) % width == sub)


def build_kernel(
    lat, coef_ref, conv_in_ref, conv_out_ref, time_ref, win_ref, noise_ref,
    w_in_ref, w_out_ref, column_ref, x_ref, n_ref, *refs,
):
    waves = refs[:GROUP]
    in_ref, out_ref, wave_ref = refs[GROUP:]
    chans, hid = conv_in_ref.shape[2:]
    width = win_ref.shape[1]
    deep = in_ref.shape[0] // 9
    rows = n_ref.shape[1]
    sub = width // GROUP
    pitch = sub + 2 * EDGE
    turn = turn_of(pitch, sub, width)
    for source, target in ((win_ref, x_ref), (noise_ref, n_ref)):
        target[:, chans // ROWS * ROWS :, :] = jnp.zeros_like(target[:, chans // ROWS * ROWS :, :])
        rolled = [roll(source[pl.ds(l, chans, stride=lat), :], pitch * l + EDGE) for l in range(lat)]
        for q in range(GROUP):
            for t, tile in enumerate(tiled(rolled, pitch, turn * q)):
                target[q, 0:chans, t * width : (t + 1) * width] = tile
    me = lax.rem(lax.axis_index("lvl"), GROUP)
    in_ref[...] = jnp.zeros_like(in_ref)
    out_ref[...] = jnp.zeros_like(out_ref)
    for b in range(3):
        for a in range(3):
            tap = 3 * b + a
            in_ref[tap * deep : tap * deep + chans, :] = conv_in_ref[a, b].astype(F32)
            out_ref[a * rows : a * rows + chans, b * hid : (b + 1) * hid] = conv_out_ref[a, b].astype(F32)
    w_in_ref[...] = jnp.transpose(in_ref[...]).astype(BF16)
    w_out_ref[...] = out_ref[...].astype(BF16)
    column_ref[...] = jnp.transpose(jnp.broadcast_to(time_ref[...], (ROWS, hid)))[:, :1]

    spread = coef_ref[2:3, 0:1]
    wave_ref[:, chans // ROWS * ROWS :, :] = jnp.zeros_like(wave_ref[:, chans // ROWS * ROWS :, :])
    for t in range(lat // GROUP):
        lines = [noise_ref[pl.ds(GROUP * t + i, chans, stride=lat), :] * spread for i in range(GROUP)]
        for q, line in enumerate(swapped(lines)):
            wave_ref[q, 0:chans, t * width : (t + 1) * width] = line
    for m in range(GROUP):
        waves[m][...] = wave_ref[lax.bitwise_xor(me, m)]


def lat_shifted(x, pitch, first):
    lane = lanes_of(x)
    slots = x.shape[1] // pitch
    zero = jnp.zeros_like(x)
    final = (first - 1) % slots
    below = jnp.where(between(lane, first * pitch, (first + 1) * pitch), zero, roll(x, pitch))
    above = jnp.where(between(lane, final * pitch, (final + 1) * pitch), zero, roll(x, -pitch))
    return below, above


def scores_of(strips, shifts, firsts, w_in_ref, w_out_ref, pitch):
    strip = strips[0].shape[1]
    rows = w_out_ref.shape[0] // 3
    stacks = []
    for x, first in zip(strips, firsts):
        x = x.astype(BF16)
        stack = []
        for moved in (roll(x, 1), x, roll(x, -1)):
            below, above = lat_shifted(moved, pitch, first)
            stack += [below, moved, above]
        stacks.append(jnp.concatenate(stack, axis=0))
    pre = jnp.dot(w_in_ref[...], jnp.concatenate(stacks, axis=1), preferred_element_type=F32)
    hiddens = []
    for i, shift in enumerate(shifts):
        value = pre[:, i * strip : (i + 1) * strip] + shift
        hidden = (value / (1.0 + jnp.exp(-value))).astype(BF16)
        hiddens.append(jnp.concatenate([roll(hidden, 1), hidden, roll(hidden, -1)], axis=0))
    out = jnp.dot(w_out_ref[...], jnp.concatenate(hiddens, axis=1), preferred_element_type=F32)
    scores = []
    for i, first in enumerate(firsts):
        lines = out[:, i * strip : (i + 1) * strip]
        below, _ = lat_shifted(lines[:rows], pitch, first)
        _, above = lat_shifted(lines[2 * rows :], pitch, first)
        scores.append(lines[rows : 2 * rows] + below + above)
    return scores


def edged(strip, edges, pitch, turn, source, target, count, chosen=None):
    width = edges.shape[1]
    lat = strip.shape[1] // pitch
    lane = lanes_of(strip)
    moves = {}
    for l in range(lat):
        slot = (l + turn) % lat
        moves.setdefault((slot * pitch + target - SLOT * l - source) % width, []).append(slot)
    for shift, slots in moves.items():
        moved = jnp.concatenate([roll(edges, shift)] * (strip.shape[1] // width), axis=1)
        mask = None
        for slot in slots:
            here = between(lane, slot * pitch + target, slot * pitch + target + count)
            mask = here if mask is None else jnp.logical_or(mask, here)
        if chosen is not None:
            mask = jnp.logical_and(mask, chosen)
        strip = jnp.where(mask, moved, strip)
    return strip


def first_kernel(lat, coef_ref, x_ref, n_ref, before_ref, after_ref, column_ref, w_in_ref, w_out_ref, *refs):
    outs = refs[:GROUP]
    (inc_ref,) = refs[GROUP:]
    rows = n_ref.shape[1]
    strip = n_ref.shape[2]
    width = before_ref.shape[1]
    sub = width // GROUP
    pitch = strip // lat
    turn = turn_of(pitch, sub, width)
    me = lax.rem(lax.axis_index("lvl"), GROUP)
    half, drift, spread, time = [coef_ref[r : r + 1, 0:1] for r in range(4)]
    shift = column_ref[...] * time
    before = before_ref[...]
    after = after_ref[...]
    tail = x_ref.shape[1] - rows
    for part in range(GROUP // 2):
        quarters = (2 * part, 2 * part + 1)
        strips = []
        others = []
        for q in quarters:
            x = x_ref[q, 0:rows]
            noise = n_ref[q]
            if q == 0:
                x = edged(x, before, pitch, turn * q, 0, 0, 4)
                noise = edged(noise, before, pitch, turn * q, 4, 2, 2)
            if q == GROUP - 1:
                x = edged(x, after, pitch, turn * q, 4, pitch - EDGE, 4)
                noise = edged(noise, after, pitch, turn * q, 0, pitch - EDGE, 2)
            strips.append(jnp.concatenate([x, jnp.zeros((tail, strip), F32)], axis=0))
            others.append(x * half + noise * spread)
        firsts = [(turn * q) % lat for q in quarters]
        scores = scores_of(strips, [shift, shift], firsts, w_in_ref, w_out_ref, pitch)
        for q, score, other in zip(quarters, scores, others):
            inc_ref[q] = roll(other + drift * score, -pitch * turn * q)
    for m in range(GROUP):
        outs[m][...] = inc_ref[lax.bitwise_xor(me, m)]


def base_kernel(lat, anchor_ref, before_ref, after_ref, *refs):
    incs = refs[:GROUP]
    base_ref, tight_ref, inc_ref, anc_ref = refs[GROUP:]
    chans = anchor_ref.shape[0] // lat
    width = anchor_ref.shape[1]
    sub = width // GROUP
    strip = base_ref.shape[2]
    pitch = strip // lat
    me = lax.rem(lax.axis_index("lvl"), GROUP)
    for m in range(GROUP):
        inc_ref[lax.bitwise_xor(me, m)] = incs[m][...]
    anc_ref[chans // ROWS * ROWS :, :] = jnp.zeros_like(anc_ref[chans // ROWS * ROWS :, :])
    tight_ref[chans // ROWS * ROWS :, :] = jnp.zeros_like(tight_ref[chans // ROWS * ROWS :, :])
    turned = []
    for l in range(lat):
        turned.append(pltpu.roll(anchor_ref[pl.ds(l, chans, stride=lat), :], lax.rem(width - me * sub, width), 1))
    for t, tile in enumerate(tiled([roll(line, pitch * l + EDGE) for l, line in enumerate(turned)], pitch, 0)):
        anc_ref[0:chans, t * width : (t + 1) * width] = tile
    block = lanes_of(turned[0]) // sub
    for t in range(lat // GROUP):
        tile = turned[GROUP * t]
        for i in range(1, GROUP):
            tile = jnp.where(block == i, roll(turned[GROUP * t + i], i * sub), tile)
        tight_ref[0:chans, t * width : (t + 1) * width] = tile
    state = edged(anc_ref[...], before_ref[...], pitch, 0, 6, 2, 2, me == 0)
    state = edged(state, after_ref[...], pitch, 0, 2, pitch - EDGE, 2, me == GROUP - 1)
    for j in range(GROUP):
        base_ref[j] = state
        if j + 1 < GROUP:
            state = state + inc_ref[j]


def second_kernel(lat, coef_ref, base_ref, column_ref, w_in_ref, w_out_ref, carry_ref, sum_ref):
    rows, strip = carry_ref.shape
    pitch = strip // lat
    width = coef_ref.shape[1]
    sub = width // GROUP
    tail = w_in_ref.shape[1] // 9 - rows
    carry = carry_ref[...]

    def packed(block):
        tiles = [block[:, t * width : (t + 1) * width] for t in range(strip // width)]
        lane = lanes_of(tiles[0])
        outs = []
        for l in range(lat):
            low = l * pitch + EDGE
            piece = tiles[low // width]
            if (low + sub - 1) // width != low // width:
                piece = jnp.where(lane >= low % width, piece, tiles[low // width + 1])
            moved = roll(piece, (l % GROUP) * sub - low)
            outs.append(moved if l % GROUP == 0 else jnp.where(lane >= (l % GROUP) * sub, moved, outs.pop()))
        return jnp.concatenate(outs, axis=1)

    running = jnp.zeros(sum_ref.shape[1:], F32)
    for part in range(GROUP // 2):
        levels = (2 * part, 2 * part + 1)
        states = [base_ref[j] + carry for j in levels]
        strips = [jnp.concatenate([x, jnp.zeros((tail, strip), F32)], axis=0) for x in states]
        coefs = [[coef_ref[COEFS * (j + 1) + r : COEFS * (j + 1) + r + 1, 0:1] for r in range(4)] for j in levels]
        shifts = [column_ref[...] * coef[3] for coef in coefs]
        scores = scores_of(strips, shifts, [0, 0], w_in_ref, w_out_ref, pitch)
        for j, x, score, coef in zip(levels, states, scores, coefs):
            running = running + packed(x * coef[0] + score * coef[1])
            sum_ref[j] = running


def share_kernel(tight_ref, sum_ref, *refs):
    waves = refs[:GROUP]
    outs = refs[GROUP : 2 * GROUP]
    total_ref, wave_ref = refs[2 * GROUP :]
    me = lax.rem(lax.axis_index("lvl"), GROUP)
    for m in range(GROUP):
        wave_ref[lax.bitwise_xor(me, m)] = waves[m][...]
    noise = jnp.zeros(total_ref.shape, F32)
    for j in range(GROUP):
        noise = noise + wave_ref[j]
        share = sum_ref[j] + noise
        wave_ref[j] = tight_ref[...] + share
    total_ref[...] = share
    for m in range(GROUP):
        outs[m][...] = wave_ref[lax.bitwise_xor(me, m)]


def last_kernel(lat, *refs):
    parts = refs[:GROUP]
    out_any, all_ref, line_ref, sems = refs[GROUP:]
    chans = line_ref.shape[0] // lat
    width = line_ref.shape[1]
    me = lax.rem(lax.axis_index("lvl"), GROUP)
    for m in range(GROUP):
        all_ref[lax.bitwise_xor(me, m)] = parts[m][...]
    size = up_to(-(-chans // 3), ROWS)
    copies = []
    for i, low in enumerate(range(0, chans, size)):
        high = min(low + size, chans)
        for t in range(lat // GROUP):
            lanes = slice(t * width, (t + 1) * width)
            lines = swapped([all_ref[q, low:high, lanes] for q in range(GROUP)])
            for k, line in enumerate(lines):
                line_ref[pl.ds(low * lat + GROUP * t + k, high - low, stride=lat), :] = line
        spot = pl.ds(low * lat, (high - low) * lat)
        copies.append(pltpu.make_async_copy(line_ref.at[spot], out_any.at[spot], sems.at[i]))
        copies[-1].start()
    for copy in copies:
        copy.wait()


def exchange(pieces):
    count = lax.axis_size("lvl")
    got = [pieces[0]]
    for m in range(1, GROUP):
        got.append(lax.ppermute(pieces[m], "lvl", [(k, k ^ m) for k in range(count)]))
    return got


def carried(total, block):
    count = lax.axis_size("lvl")
    blocks = count // GROUP
    carry = jnp.zeros_like(total)
    for s in range(1, blocks):
        moved = lax.ppermute(total, "lvl", [(k, (k + s * GROUP) % count) for k in range(count)])
        carry = carry + jnp.where(block >= s, moved, 0.0)
    return carry


def body(window, anchor, noise, conv_in, conv_out, time_shift, plan, start):
    _, lat, chans, width = window.shape
    hid = conv_in.shape[2]
    block = lax.axis_index("lvl") // GROUP
    sub = width // GROUP
    strip = lat * (sub + 2 * EDGE)
    rows = up_to(chans, ROWS)
    deep = up_to(chans, PACK)

    def native(x):
        return jnp.transpose(x.reshape(lat, chans, width), (1, 0, 2)).reshape(chans * lat, width)

    edge = (rows, SLOT * lat)
    wide = (rows, strip)
    tight = (rows, lat * sub)
    flops = 2 * 9 * chans * hid * 2 * lat * width
    taps = jax.ShapeDtypeStruct((3, 3, chans, hid), BF16)
    first, last, coefs, win, noi, anc, taps_in, taps_out, time = call(
        functools.partial(edges_kernel, lat),
        [edge, edge, (COEFS * (GROUP + 1), width)] + [(chans * lat, width)] * 3 + [taps, taps, (1, hid)],
        [SM] + [HBM] * 7,
        [
            pltpu.SMEM(plan.shape, plan.dtype),
            pltpu.SemaphoreType.DMA((7,)),
        ],
        1 << 20,
        8,
    )(
        start,
        *(
            pltpu.with_memory_space_constraint(x, pltpu.HBM)
            for x in (
                plan,
                native(window),
                native(noise),
                native(anchor),
                jnp.swapaxes(conv_in, 2, 3),
                conv_out,
                time_shift.reshape(1, hid),
            )
        )
    )
    count = lax.axis_size("lon")
    before = lax.ppermute(last, "lon", [(k, (k + 1) % count) for k in range(count)])
    after = lax.ppermute(first, "lon", [((k + 1) % count, k) for k in range(count)])
    w_in, w_out, column, x, n, *waves = call(
        functools.partial(build_kernel, lat),
        [
            jax.ShapeDtypeStruct((hid, 9 * deep), BF16),
            jax.ShapeDtypeStruct((3 * rows, 3 * hid), BF16),
            jax.ShapeDtypeStruct((hid, 1), F32),
            (GROUP, deep, strip),
            (GROUP,) + wide,
        ]
        + [tight] * GROUP,
        [VM] * 6,
        [
            pltpu.VMEM((9 * deep, hid), F32),
            pltpu.VMEM((3 * rows, 3 * hid), F32),
            pltpu.VMEM((GROUP,) + tight, F32),
        ],
        flops // 4,
        12,
    )(coefs, taps_in, taps_out, time, win, noi)
    incs = call(
        functools.partial(first_kernel, lat),
        [wide] * GROUP,
        [VM] * 8,
        [pltpu.VMEM((GROUP,) + wide, F32)],
        flops,
        20,
    )(coefs, x, n, before, after, column, w_in, w_out)
    incs = exchange(incs)
    total = incs[0] + incs[1] + incs[2] + incs[3]
    carry = carried(total, block)
    waves = exchange(waves)
    base, packed = call(
        functools.partial(base_kernel, lat),
        [(GROUP,) + wide, tight],
        [VM] * (3 + GROUP),
        [pltpu.VMEM((GROUP,) + wide, F32), pltpu.VMEM(wide, F32)],
        flops // 4,
        12,
    )(anc, before, after, *incs)
    (sums,) = call(
        functools.partial(second_kernel, lat),
        [(GROUP,) + tight],
        [VM] * 6,
        [],
        flops,
        20,
    )(coefs, base, column, w_in, w_out, carry)
    done = call(
        share_kernel,
        [tight] * (GROUP + 1),
        [VM] * (2 + GROUP),
        [pltpu.VMEM((GROUP,) + tight, F32)],
        1 << 20,
        4,
    )(packed, sums, *waves)
    carry = carried(done[GROUP], block)
    parts = exchange([part + carry for part in done[:GROUP]])
    (out,) = call(
        functools.partial(last_kernel, lat),
        [(chans * lat, width)],
        [VM] * GROUP,
        [pltpu.VMEM((GROUP,) + tight, F32), pltpu.VMEM((chans * lat, width), F32), pltpu.SemaphoreType.DMA((3,))],
        1 << 20,
        8,
        [HBM],
    )(*parts)
    return jnp.transpose(out.reshape(chans, lat, width), (1, 0, 2))[None]


def solution(mesh):
    return jax.shard_map(
        body,
        mesh=mesh,
        in_specs=(
            P("lvl", None, None, "lon"),
            P(None, None, "lon"),
            P("lvl", None, None, "lon"),
            P(),
            P(),
            P(),
            P(),
            P(),
        ),
        out_specs=P("lvl", None, None, "lon"),
        check_vma=False,
    )
```

```python
import functools

import jax
import jax.numpy as jnp
from jax import lax
from jax.experimental import pallas as pl
from jax.experimental.pallas import tpu as pltpu
from jax.sharding import PartitionSpec as P


GROUP = 4
EDGE = 4
SLOT = 2 * EDGE
ROWS = 8
PACK = 16
COEFS = 8

VM = pl.BlockSpec(memory_space=pltpu.VMEM)
SM = pl.BlockSpec(memory_space=pltpu.SMEM)
HBM = pl.BlockSpec(memory_space=pltpu.HBM)
F32 = jnp.float32
BF16 = jnp.bfloat16


def up_to(value, unit):
    return -(-value // unit) * unit


def call(kernel, outs, specs, scratch, flops, limit, out_specs=None):
    outs = [out if isinstance(out, jax.ShapeDtypeStruct) else jax.ShapeDtypeStruct(out, F32) for out in outs]
    return pl.pallas_call(
        kernel,
        out_shape=outs,
        in_specs=specs,
        out_specs=out_specs or [VM] * len(outs),
        scratch_shapes=scratch,
        compiler_params=pltpu.CompilerParams(vmem_limit_bytes=int(limit * (1 << 20))),
        cost_estimate=pl.CostEstimate(flops=flops, bytes_accessed=4 << 20, transcendentals=0),
    )


def roll(x, shift):
    shift = shift % x.shape[1]
    return pltpu.roll(x, shift, 1) if shift else x


def lanes_of(x):
    return lax.broadcasted_iota(jnp.int32, x.shape, 1)


def place():
    level = lax.axis_index("lvl")
    mine = lax.rem(level, GROUP)
    return mine, lax.bitwise_xor(mine, lax.rem(level // GROUP, 2) * (GROUP // 2))


def between(lane, low, high):
    return jnp.logical_and(lane >= low, lane < high)


def swapped(arrays):
    count = len(arrays)
    sub = arrays[0].shape[1] // count
    block = lanes_of(arrays[0]) // sub
    turned = []
    for r in range(count):
        mixed = arrays[r]
        for j in range(1, count):
            mixed = jnp.where(block == j, arrays[(j + r) % count], mixed)
        turned.append(roll(mixed, r * sub))
    outs = []
    for j in range(count):
        mixed = turned[(0 - j) % count]
        for i in range(1, count):
            mixed = jnp.where(block == i, turned[(i - j) % count], mixed)
        outs.append(mixed)
    return outs


def coefs_of(plan_ref, entry):
    now = plan_ref[entry].astype(F32)
    later = plan_ref[entry + 1].astype(F32)
    beta = 0.1 + 19.9 * now / 1000.0
    step = (now - later) / 1000.0
    return [0.5 * beta * step, beta * step, jnp.sqrt(jnp.full((1, 1), beta * step, F32)), now / 1000.0]


def edges_kernel(
    lat, start_ref, plan_hbm, win_hbm, noise_hbm, anchor_hbm, conv_in_hbm, conv_out_hbm, time_hbm,
    first_ref, last_ref, coef_ref, win_ref, noise_ref, anchor_ref, conv_in_ref, conv_out_ref, time_ref,
    plan_ref, sems,
):
    pairs = [
        (plan_hbm, plan_ref),
        (win_hbm, win_ref),
        (noise_hbm, noise_ref),
        (anchor_hbm, anchor_ref),
        (conv_in_hbm, conv_in_ref),
        (conv_out_hbm, conv_out_ref),
        (time_hbm, time_ref),
    ]
    copies = [pltpu.make_async_copy(source, target, sems.at[i]) for i, (source, target) in enumerate(pairs)]
    for copy in copies:
        copy.start()
    copies[0].wait()
    copies = copies[1:]
    level = lax.axis_index("lvl")
    entries = [level] + [level - lax.rem(level, GROUP) + j for j in range(GROUP)]
    for i, entry in enumerate(entries):
        values = coefs_of(plan_ref, start_ref[0] + entry)
        for r, value in enumerate(values):
            coef_ref[COEFS * i + r : COEFS * i + r + 1, :] = jnp.broadcast_to(
                value if r == 2 else jnp.full((1, 1), value, F32), (1, coef_ref.shape[1])
            )
    chans = win_ref.shape[0] // lat
    tiles = []
    for copy, ref, shift, skip in zip(copies, (win_ref, noise_ref, anchor_ref), (4, 6, 8), (0, 0, 6)):
        copy.wait()
        tile = roll(ref[pl.ds(0, chans, stride=lat), :], shift)
        width = tile.shape[1]
        slot = lax.rem(lanes_of(tile) + width - skip, width) // SLOT
        for l in range(1, lat):
            tile = jnp.where(slot == l, roll(ref[pl.ds(l, chans, stride=lat), :], SLOT * l + shift), tile)
        tiles.append(tile)
    win, noise, anchor = tiles
    spot = lax.rem(lanes_of(win), SLOT)
    last = jnp.where(spot < 4, win, jnp.where(spot < 6, noise, anchor))
    first = jnp.where(spot < 2, roll(noise, -6), jnp.where(spot < 4, roll(anchor, -6), win))
    for ref, value in ((first_ref, first), (last_ref, last)):
        ref[...] = jnp.zeros_like(ref)
        ref[0:chans, :] = value
    for copy in copies[3:]:
        copy.wait()


def tiled(rolled, pitch, turn):
    lat = len(rolled)
    width = rolled[0].shape[1]
    lane = lanes_of(rolled[0])
    tiles = []
    for t in range(lat * pitch // width):
        tile = None
        for slot in range(lat):
            low = slot * pitch - t * width
            if low >= width or low + pitch <= 0:
                continue
            piece = rolled[(slot - turn) % lat]
            tile = piece if tile is None else jnp.where(lane >= low, piece, tile)
        tiles.append(tile)
    return tiles


def turn_of(pitch, sub, width):
    return next(k for k in range(width) if (pitch * k) % width == sub)


def build_kernel(
    lat, coef_ref, conv_in_ref, conv_out_ref, time_ref, win_ref, noise_ref,
    w_in_ref, w_out_ref, column_ref, x_ref, n_ref, *refs,
):
    waves = refs[:GROUP]
    in_ref, out_ref, wave_ref = refs[GROUP:]
    chans, hid = conv_in_ref.shape[2:]
    width = win_ref.shape[1]
    deep = in_ref.shape[0] // 9
    rows = n_ref.shape[1]
    sub = width // GROUP
    pitch = sub + 2 * EDGE
    turn = turn_of(pitch, sub, width)
    for source, target in ((win_ref, x_ref), (noise_ref, n_ref)):
        target[:, chans // ROWS * ROWS :, :] = jnp.zeros_like(target[:, chans // ROWS * ROWS :, :])
        rolled = [roll(source[pl.ds(l, chans, stride=lat), :], pitch * l + EDGE) for l in range(lat)]
        for q in range(GROUP):
            for t, tile in enumerate(tiled(rolled, pitch, turn * q)):
                target[q, 0:chans, t * width : (t + 1) * width] = tile
    _, quarter = place()
    in_ref[...] = jnp.zeros_like(in_ref)
    out_ref[...] = jnp.zeros_like(out_ref)
    for b in range(3):
        for a in range(3):
            tap = 3 * b + a
            in_ref[tap * deep : tap * deep + chans, :] = conv_in_ref[a, b].astype(F32)
            out_ref[a * rows : a * rows + chans, b * hid : (b + 1) * hid] = conv_out_ref[a, b].astype(F32)
    w_in_ref[...] = jnp.transpose(in_ref[...]).astype(BF16)
    w_out_ref[...] = out_ref[...].astype(BF16)
    column_ref[...] = jnp.transpose(jnp.broadcast_to(time_ref[...], (ROWS, hid)))[:, :1]

    spread = coef_ref[2:3, 0:1]
    wave_ref[:, chans // ROWS * ROWS :, :] = jnp.zeros_like(wave_ref[:, chans // ROWS * ROWS :, :])
    for t in range(lat // GROUP):
        lines = [noise_ref[pl.ds(GROUP * t + i, chans, stride=lat), :] * spread for i in range(GROUP)]
        for q, line in enumerate(swapped(lines)):
            wave_ref[q, 0:chans, t * width : (t + 1) * width] = line
    for m in range(GROUP):
        waves[m][...] = wave_ref[lax.bitwise_xor(quarter, m)]


def lat_shifted(x, pitch, first):
    lane = lanes_of(x)
    slots = x.shape[1] // pitch
    zero = jnp.zeros_like(x)
    final = (first - 1) % slots
    below = jnp.where(between(lane, first * pitch, (first + 1) * pitch), zero, roll(x, pitch))
    above = jnp.where(between(lane, final * pitch, (final + 1) * pitch), zero, roll(x, -pitch))
    return below, above


def scores_of(strips, shifts, firsts, w_in_ref, w_out_ref, pitch):
    strip = strips[0].shape[1]
    rows = w_out_ref.shape[0] // 3
    stacks = []
    for x, first in zip(strips, firsts):
        x = x.astype(BF16)
        stack = []
        for moved in (roll(x, 1), x, roll(x, -1)):
            below, above = lat_shifted(moved, pitch, first)
            stack += [below, moved, above]
        stacks.append(jnp.concatenate(stack, axis=0))
    pre = jnp.dot(w_in_ref[...], jnp.concatenate(stacks, axis=1), preferred_element_type=F32)
    hiddens = []
    for i, shift in enumerate(shifts):
        value = pre[:, i * strip : (i + 1) * strip] + shift
        hidden = (value / (1.0 + jnp.exp(-value))).astype(BF16)
        hiddens.append(jnp.concatenate([roll(hidden, 1), hidden, roll(hidden, -1)], axis=0))
    out = jnp.dot(w_out_ref[...], jnp.concatenate(hiddens, axis=1), preferred_element_type=F32)
    scores = []
    for i, first in enumerate(firsts):
        lines = out[:, i * strip : (i + 1) * strip]
        below, _ = lat_shifted(lines[:rows], pitch, first)
        _, above = lat_shifted(lines[2 * rows :], pitch, first)
        scores.append(lines[rows : 2 * rows] + below + above)
    return scores


def edged(strip, edges, pitch, turn, source, target, count, chosen=None):
    width = edges.shape[1]
    lat = strip.shape[1] // pitch
    lane = lanes_of(strip)
    moves = {}
    for l in range(lat):
        slot = (l + turn) % lat
        moves.setdefault((slot * pitch + target - SLOT * l - source) % width, []).append(slot)
    for shift, slots in moves.items():
        moved = jnp.concatenate([roll(edges, shift)] * (strip.shape[1] // width), axis=1)
        mask = None
        for slot in slots:
            here = between(lane, slot * pitch + target, slot * pitch + target + count)
            mask = here if mask is None else jnp.logical_or(mask, here)
        if chosen is not None:
            mask = jnp.logical_and(mask, chosen)
        strip = jnp.where(mask, moved, strip)
    return strip


def first_kernel(lat, coef_ref, x_ref, n_ref, before_ref, after_ref, column_ref, w_in_ref, w_out_ref, *refs):
    outs = refs[:GROUP]
    (inc_ref,) = refs[GROUP:]
    rows = n_ref.shape[1]
    strip = n_ref.shape[2]
    width = before_ref.shape[1]
    sub = width // GROUP
    pitch = strip // lat
    turn = turn_of(pitch, sub, width)
    _, quarter = place()
    half, drift, spread, time = [coef_ref[r : r + 1, 0:1] for r in range(4)]
    shift = column_ref[...] * time
    before = before_ref[...]
    after = after_ref[...]
    tail = x_ref.shape[1] - rows
    for part in range(GROUP // 2):
        quarters = (2 * part, 2 * part + 1)
        strips = []
        others = []
        for q in quarters:
            x = x_ref[q, 0:rows]
            noise = n_ref[q]
            if q == 0:
                x = edged(x, before, pitch, turn * q, 0, 0, 4)
                noise = edged(noise, before, pitch, turn * q, 4, 2, 2)
            if q == GROUP - 1:
                x = edged(x, after, pitch, turn * q, 4, pitch - EDGE, 4)
                noise = edged(noise, after, pitch, turn * q, 0, pitch - EDGE, 2)
            strips.append(jnp.concatenate([x, jnp.zeros((tail, strip), F32)], axis=0))
            others.append(x * half + noise * spread)
        firsts = [(turn * q) % lat for q in quarters]
        scores = scores_of(strips, [shift, shift], firsts, w_in_ref, w_out_ref, pitch)
        for q, score, other in zip(quarters, scores, others):
            inc_ref[q] = roll(other + drift * score, -pitch * turn * q)
    for m in range(GROUP):
        outs[m][...] = inc_ref[lax.bitwise_xor(quarter, m)]


def base_kernel(lat, anchor_ref, before_ref, after_ref, *refs):
    incs = refs[:GROUP]
    base_ref, tight_ref, inc_ref, anc_ref = refs[GROUP:]
    chans = anchor_ref.shape[0] // lat
    width = anchor_ref.shape[1]
    sub = width // GROUP
    strip = base_ref.shape[2]
    pitch = strip // lat
    mine, quarter = place()
    for m in range(GROUP):
        inc_ref[lax.bitwise_xor(mine, m)] = incs[m][...]
    anc_ref[chans // ROWS * ROWS :, :] = jnp.zeros_like(anc_ref[chans // ROWS * ROWS :, :])
    tight_ref[chans // ROWS * ROWS :, :] = jnp.zeros_like(tight_ref[chans // ROWS * ROWS :, :])
    turned = []
    for l in range(lat):
        turned.append(pltpu.roll(anchor_ref[pl.ds(l, chans, stride=lat), :], lax.rem(width - quarter * sub, width), 1))
    for t, tile in enumerate(tiled([roll(line, pitch * l + EDGE) for l, line in enumerate(turned)], pitch, 0)):
        anc_ref[0:chans, t * width : (t + 1) * width] = tile
    block = lanes_of(turned[0]) // sub
    for t in range(lat // GROUP):
        tile = turned[GROUP * t]
        for i in range(1, GROUP):
            tile = jnp.where(block == i, roll(turned[GROUP * t + i], i * sub), tile)
        tight_ref[0:chans, t * width : (t + 1) * width] = tile
    state = edged(anc_ref[...], before_ref[...], pitch, 0, 6, 2, 2, quarter == 0)
    state = edged(state, after_ref[...], pitch, 0, 2, pitch - EDGE, 2, quarter == GROUP - 1)
    for j in range(GROUP):
        base_ref[j] = state
        if j + 1 < GROUP:
            state = state + inc_ref[j]


def second_kernel(lat, coef_ref, base_ref, column_ref, w_in_ref, w_out_ref, carry_ref, sum_ref):
    rows, strip = carry_ref.shape
    pitch = strip // lat
    width = coef_ref.shape[1]
    sub = width // GROUP
    tail = w_in_ref.shape[1] // 9 - rows
    carry = carry_ref[...]

    def packed(block):
        tiles = [block[:, t * width : (t + 1) * width] for t in range(strip // width)]
        lane = lanes_of(tiles[0])
        outs = []
        for l in range(lat):
            low = l * pitch + EDGE
            piece = tiles[low // width]
            if (low + sub - 1) // width != low // width:
                piece = jnp.where(lane >= low % width, piece, tiles[low // width + 1])
            moved = roll(piece, (l % GROUP) * sub - low)
            outs.append(moved if l % GROUP == 0 else jnp.where(lane >= (l % GROUP) * sub, moved, outs.pop()))
        return jnp.concatenate(outs, axis=1)

    running = jnp.zeros(sum_ref.shape[1:], F32)
    for part in range(GROUP // 2):
        levels = (2 * part, 2 * part + 1)
        states = [base_ref[j] + carry for j in levels]
        strips = [jnp.concatenate([x, jnp.zeros((tail, strip), F32)], axis=0) for x in states]
        coefs = [[coef_ref[COEFS * (j + 1) + r : COEFS * (j + 1) + r + 1, 0:1] for r in range(4)] for j in levels]
        shifts = [column_ref[...] * coef[3] for coef in coefs]
        scores = scores_of(strips, shifts, [0, 0], w_in_ref, w_out_ref, pitch)
        for j, x, score, coef in zip(levels, states, scores, coefs):
            running = running + packed(x * coef[0] + score * coef[1])
            sum_ref[j] = running


def share_kernel(tight_ref, sum_ref, *refs):
    waves = refs[:GROUP]
    outs = refs[GROUP : 2 * GROUP]
    total_ref, wave_ref = refs[2 * GROUP :]
    mine, _ = place()
    for m in range(GROUP):
        wave_ref[lax.bitwise_xor(mine, m)] = waves[m][...]
    noise = jnp.zeros(total_ref.shape, F32)
    for j in range(GROUP):
        noise = noise + wave_ref[j]
        share = sum_ref[j] + noise
        wave_ref[j] = tight_ref[...] + share
    total_ref[...] = share
    for m in range(GROUP):
        outs[m][...] = wave_ref[lax.bitwise_xor(mine, m)]


def last_kernel(lat, *refs):
    parts = refs[:GROUP]
    out_any, all_ref, line_ref, sems = refs[GROUP:]
    chans = line_ref.shape[0] // lat
    width = line_ref.shape[1]
    _, quarter = place()
    for m in range(GROUP):
        all_ref[lax.bitwise_xor(quarter, m)] = parts[m][...]
    size = up_to(-(-chans // 3), ROWS)
    copies = []
    for i, low in enumerate(range(0, chans, size)):
        high = min(low + size, chans)
        for t in range(lat // GROUP):
            lanes = slice(t * width, (t + 1) * width)
            lines = swapped([all_ref[q, low:high, lanes] for q in range(GROUP)])
            for k, line in enumerate(lines):
                line_ref[pl.ds(low * lat + GROUP * t + k, high - low, stride=lat), :] = line
        spot = pl.ds(low * lat, (high - low) * lat)
        copies.append(pltpu.make_async_copy(line_ref.at[spot], out_any.at[spot], sems.at[i]))
        copies[-1].start()
    for copy in copies:
        copy.wait()


def exchange(pieces):
    count = lax.axis_size("lvl")
    got = [pieces[0]]
    for m in range(1, GROUP):
        got.append(lax.ppermute(pieces[m], "lvl", [(k, k ^ m) for k in range(count)]))
    return got


def carried(total, block):
    count = lax.axis_size("lvl")
    blocks = count // GROUP
    carry = jnp.zeros_like(total)
    for s in range(1, blocks):
        pairs = []
        for k in range(count):
            target = (k // GROUP + s) % blocks
            turn = (k // GROUP + target) % 2 * (GROUP // 2)
            pairs.append((k, target * GROUP + (k % GROUP ^ turn)))
        moved = lax.ppermute(total, "lvl", pairs)
        carry = carry + jnp.where(block >= s, moved, 0.0)
    return carry


def body(window, anchor, noise, conv_in, conv_out, time_shift, plan, start):
    _, lat, chans, width = window.shape
    hid = conv_in.shape[2]
    block = lax.axis_index("lvl") // GROUP
    sub = width // GROUP
    strip = lat * (sub + 2 * EDGE)
    rows = up_to(chans, ROWS)
    deep = up_to(chans, PACK)

    def native(x):
        return jnp.transpose(x.reshape(lat, chans, width), (1, 0, 2)).reshape(chans * lat, width)

    edge = (rows, SLOT * lat)
    wide = (rows, strip)
    tight = (rows, lat * sub)
    flops = 2 * 9 * chans * hid * 2 * lat * width
    taps = jax.ShapeDtypeStruct((3, 3, chans, hid), BF16)
    first, last, coefs, win, noi, anc, taps_in, taps_out, time = call(
        functools.partial(edges_kernel, lat),
        [edge, edge, (COEFS * (GROUP + 1), width)] + [(chans * lat, width)] * 3 + [taps, taps, (1, hid)],
        [SM] + [HBM] * 7,
        [
            pltpu.SMEM(plan.shape, plan.dtype),
            pltpu.SemaphoreType.DMA((7,)),
        ],
        1 << 20,
        8,
    )(
        start,
        *(
            pltpu.with_memory_space_constraint(x, pltpu.HBM)
            for x in (
                plan,
                native(window),
                native(noise),
                native(anchor),
                jnp.swapaxes(conv_in, 2, 3),
                conv_out,
                time_shift.reshape(1, hid),
            )
        )
    )
    count = lax.axis_size("lon")
    before = lax.ppermute(last, "lon", [(k, (k + 1) % count) for k in range(count)])
    after = lax.ppermute(first, "lon", [((k + 1) % count, k) for k in range(count)])
    w_in, w_out, column, x, n, *waves = call(
        functools.partial(build_kernel, lat),
        [
            jax.ShapeDtypeStruct((hid, 9 * deep), BF16),
            jax.ShapeDtypeStruct((3 * rows, 3 * hid), BF16),
            jax.ShapeDtypeStruct((hid, 1), F32),
            (GROUP, deep, strip),
            (GROUP,) + wide,
        ]
        + [tight] * GROUP,
        [VM] * 6,
        [
            pltpu.VMEM((9 * deep, hid), F32),
            pltpu.VMEM((3 * rows, 3 * hid), F32),
            pltpu.VMEM((GROUP,) + tight, F32),
        ],
        flops // 4,
        12,
    )(coefs, taps_in, taps_out, time, win, noi)
    incs = call(
        functools.partial(first_kernel, lat),
        [wide] * GROUP,
        [VM] * 8,
        [pltpu.VMEM((GROUP,) + wide, F32)],
        flops,
        20,
    )(coefs, x, n, before, after, column, w_in, w_out)
    incs = exchange(incs)
    total = incs[0] + incs[1] + incs[2] + incs[3]
    carry = carried(total, block)
    waves = exchange(waves)
    base, packed = call(
        functools.partial(base_kernel, lat),
        [(GROUP,) + wide, tight],
        [VM] * (3 + GROUP),
        [pltpu.VMEM((GROUP,) + wide, F32), pltpu.VMEM(wide, F32)],
        flops // 4,
        12,
    )(anc, before, after, *incs)
    (sums,) = call(
        functools.partial(second_kernel, lat),
        [(GROUP,) + tight],
        [VM] * 6,
        [],
        flops,
        20,
    )(coefs, base, column, w_in, w_out, carry)
    done = call(
        share_kernel,
        [tight] * (GROUP + 1),
        [VM] * (2 + GROUP),
        [pltpu.VMEM((GROUP,) + tight, F32)],
        1 << 20,
        4,
    )(packed, sums, *waves)
    carry = carried(done[GROUP], block)
    parts = exchange([part + carry for part in done[:GROUP]])
    (out,) = call(
        functools.partial(last_kernel, lat),
        [(chans * lat, width)],
        [VM] * GROUP,
        [pltpu.VMEM((GROUP,) + tight, F32), pltpu.VMEM((chans * lat, width), F32), pltpu.SemaphoreType.DMA((3,))],
        1 << 20,
        8,
        [HBM],
    )(*parts)
    return jnp.transpose(out.reshape(chans, lat, width), (1, 0, 2))[None]


def solution(mesh):
    return jax.shard_map(
        body,
        mesh=mesh,
        in_specs=(
            P("lvl", None, None, "lon"),
            P(None, None, "lon"),
            P("lvl", None, None, "lon"),
            P(),
            P(),
            P(),
            P(),
            P(),
        ),
        out_specs=P("lvl", None, None, "lon"),
        check_vma=False,
    )
```

```python
import functools

import jax
import jax.numpy as jnp
from jax import lax
from jax.experimental import pallas as pl
from jax.experimental.pallas import tpu as pltpu
from jax.sharding import PartitionSpec as P


GROUP = 4
EDGE = 4
SLOT = 2 * EDGE
ROWS = 8
PACK = 16
COEFS = 8

VM = pl.BlockSpec(memory_space=pltpu.VMEM)
SM = pl.BlockSpec(memory_space=pltpu.SMEM)
HBM = pl.BlockSpec(memory_space=pltpu.HBM)
F32 = jnp.float32
BF16 = jnp.bfloat16


def up_to(value, unit):
    return -(-value // unit) * unit


def call(kernel, outs, specs, scratch, flops, limit, out_specs=None):
    outs = [out if isinstance(out, jax.ShapeDtypeStruct) else jax.ShapeDtypeStruct(out, F32) for out in outs]
    return pl.pallas_call(
        kernel,
        out_shape=outs,
        in_specs=specs,
        out_specs=out_specs or [VM] * len(outs),
        scratch_shapes=scratch,
        compiler_params=pltpu.CompilerParams(vmem_limit_bytes=int(limit * (1 << 20))),
        cost_estimate=pl.CostEstimate(flops=flops, bytes_accessed=4 << 20, transcendentals=0),
    )


def roll(x, shift):
    shift = shift % x.shape[1]
    return pltpu.roll(x, shift, 1) if shift else x


def lanes_of(x):
    return lax.broadcasted_iota(jnp.int32, x.shape, 1)


def place():
    level = lax.axis_index("lvl")
    mine = lax.rem(level, GROUP)
    return mine, lax.bitwise_xor(mine, lax.rem(level // GROUP, 2) * (GROUP // 2))


def between(lane, low, high):
    return jnp.logical_and(lane >= low, lane < high)


def swapped(arrays):
    count = len(arrays)
    sub = arrays[0].shape[1] // count
    block = lanes_of(arrays[0]) // sub
    turned = []
    for r in range(count):
        mixed = arrays[r]
        for j in range(1, count):
            mixed = jnp.where(block == j, arrays[(j + r) % count], mixed)
        turned.append(roll(mixed, r * sub))
    outs = []
    for j in range(count):
        mixed = turned[(0 - j) % count]
        for i in range(1, count):
            mixed = jnp.where(block == i, turned[(i - j) % count], mixed)
        outs.append(mixed)
    return outs


def coefs_of(plan_ref, entry):
    now = plan_ref[entry].astype(F32)
    later = plan_ref[entry + 1].astype(F32)
    beta = 0.1 + 19.9 * now / 1000.0
    step = (now - later) / 1000.0
    return [0.5 * beta * step, beta * step, jnp.sqrt(jnp.full((1, 1), beta * step, F32)), now / 1000.0]


def edges_kernel(
    lat, start_ref, plan_hbm, win_hbm, noise_hbm, anchor_hbm, conv_in_hbm, conv_out_hbm, time_hbm,
    first_ref, last_ref, coef_ref, win_ref, noise_ref, anchor_ref, conv_in_ref, conv_out_ref, time_ref,
    plan_ref, sems,
):
    pairs = [
        (plan_hbm, plan_ref),
        (win_hbm, win_ref),
        (noise_hbm, noise_ref),
        (anchor_hbm, anchor_ref),
        (conv_in_hbm, conv_in_ref),
        (conv_out_hbm, conv_out_ref),
        (time_hbm, time_ref),
    ]
    copies = [pltpu.make_async_copy(source, target, sems.at[i]) for i, (source, target) in enumerate(pairs)]
    for copy in copies:
        copy.start()
    copies[0].wait()
    copies = copies[1:]
    level = lax.axis_index("lvl")
    entries = [level] + [level - lax.rem(level, GROUP) + j for j in range(GROUP)]
    for i, entry in enumerate(entries):
        values = coefs_of(plan_ref, start_ref[0] + entry)
        for r, value in enumerate(values):
            coef_ref[COEFS * i + r : COEFS * i + r + 1, :] = jnp.broadcast_to(
                value if r == 2 else jnp.full((1, 1), value, F32), (1, coef_ref.shape[1])
            )
    chans = win_ref.shape[0] // lat
    tiles = []
    for copy, ref, shift, skip in zip(copies, (win_ref, noise_ref, anchor_ref), (4, 6, 8), (0, 0, 6)):
        copy.wait()
        tile = roll(ref[pl.ds(0, chans, stride=lat), :], shift)
        width = tile.shape[1]
        slot = lax.rem(lanes_of(tile) + width - skip, width) // SLOT
        for l in range(1, lat):
            tile = jnp.where(slot == l, roll(ref[pl.ds(l, chans, stride=lat), :], SLOT * l + shift), tile)
        tiles.append(tile)
    win, noise, anchor = tiles
    spot = lax.rem(lanes_of(win), SLOT)
    last = jnp.where(spot < 4, win, jnp.where(spot < 6, noise, anchor))
    first = jnp.where(spot < 2, roll(noise, -6), jnp.where(spot < 4, roll(anchor, -6), win))
    for ref, value in ((first_ref, first), (last_ref, last)):
        ref[...] = jnp.zeros_like(ref)
        ref[0:chans, :] = value
    for copy in copies[3:]:
        copy.wait()


def tiled(rolled, pitch, turn):
    lat = len(rolled)
    width = rolled[0].shape[1]
    lane = lanes_of(rolled[0])
    tiles = []
    for t in range(lat * pitch // width):
        tile = None
        for slot in range(lat):
            low = slot * pitch - t * width
            if low >= width or low + pitch <= 0:
                continue
            piece = rolled[(slot - turn) % lat]
            tile = piece if tile is None else jnp.where(lane >= low, piece, tile)
        tiles.append(tile)
    return tiles


def turn_of(pitch, sub, width):
    return next(k for k in range(width) if (pitch * k) % width == sub)


def build_kernel(
    lat, coef_ref, conv_in_ref, conv_out_ref, time_ref, win_ref, noise_ref,
    w_in_ref, w_out_ref, column_ref, x_ref, n_ref, *refs,
):
    waves = refs[:GROUP]
    in_ref, out_ref, wave_ref = refs[GROUP:]
    chans, hid = conv_in_ref.shape[2:]
    width = win_ref.shape[1]
    deep = in_ref.shape[0] // 9
    rows = n_ref.shape[1]
    sub = width // GROUP
    pitch = sub + 2 * EDGE
    turn = turn_of(pitch, sub, width)
    for source, target in ((win_ref, x_ref), (noise_ref, n_ref)):
        target[:, chans // ROWS * ROWS :, :] = jnp.zeros_like(target[:, chans // ROWS * ROWS :, :])
        rolled = [roll(source[pl.ds(l, chans, stride=lat), :], pitch * l + EDGE) for l in range(lat)]
        for q in range(GROUP):
            for t, tile in enumerate(tiled(rolled, pitch, turn * q)):
                target[q, 0:chans, t * width : (t + 1) * width] = tile
    _, quarter = place()
    in_ref[...] = jnp.zeros_like(in_ref)
    out_ref[...] = jnp.zeros_like(out_ref)
    for b in range(3):
        for a in range(3):
            tap = 3 * b + a
            in_ref[tap * deep : tap * deep + chans, :] = conv_in_ref[a, b].astype(F32)
            out_ref[a * rows : a * rows + chans, b * hid : (b + 1) * hid] = conv_out_ref[a, b].astype(F32)
    w_in_ref[...] = jnp.transpose(in_ref[...]).astype(BF16)
    w_out_ref[...] = out_ref[...].astype(BF16)
    column_ref[...] = jnp.transpose(jnp.broadcast_to(time_ref[...], (ROWS, hid)))[:, :1]

    spread = coef_ref[2:3, 0:1]
    wave_ref[:, chans // ROWS * ROWS :, :] = jnp.zeros_like(wave_ref[:, chans // ROWS * ROWS :, :])
    for t in range(lat // GROUP):
        lines = [noise_ref[pl.ds(GROUP * t + i, chans, stride=lat), :] * spread for i in range(GROUP)]
        for q, line in enumerate(swapped(lines)):
            wave_ref[q, 0:chans, t * width : (t + 1) * width] = line
    for m in range(GROUP):
        waves[m][...] = wave_ref[lax.bitwise_xor(quarter, m)]


def lat_shifted(x, pitch, first):
    lane = lanes_of(x)
    slots = x.shape[1] // pitch
    zero = jnp.zeros_like(x)
    final = (first - 1) % slots
    below = jnp.where(between(lane, first * pitch, (first + 1) * pitch), zero, roll(x, pitch))
    above = jnp.where(between(lane, final * pitch, (final + 1) * pitch), zero, roll(x, -pitch))
    return below, above


def scores_of(strips, shifts, firsts, w_in_ref, w_out_ref, pitch):
    strip = strips[0].shape[1]
    rows = w_out_ref.shape[0] // 3
    stacks = []
    for x, first in zip(strips, firsts):
        x = x.astype(BF16)
        stack = []
        for moved in (roll(x, 1), x, roll(x, -1)):
            below, above = lat_shifted(moved, pitch, first)
            stack += [below, moved, above]
        stacks.append(jnp.concatenate(stack, axis=0))
    pre = jnp.dot(w_in_ref[...], jnp.concatenate(stacks, axis=1), preferred_element_type=F32)
    hiddens = []
    for i, shift in enumerate(shifts):
        value = pre[:, i * strip : (i + 1) * strip] + shift
        hidden = (value / (1.0 + jnp.exp(-value))).astype(BF16)
        hiddens.append(jnp.concatenate([roll(hidden, 1), hidden, roll(hidden, -1)], axis=0))
    out = jnp.dot(w_out_ref[...], jnp.concatenate(hiddens, axis=1), preferred_element_type=F32)
    scores = []
    for i, first in enumerate(firsts):
        lines = out[:, i * strip : (i + 1) * strip]
        below, _ = lat_shifted(lines[:rows], pitch, first)
        _, above = lat_shifted(lines[2 * rows :], pitch, first)
        scores.append(lines[rows : 2 * rows] + below + above)
    return scores


def edged(strip, edges, pitch, turn, source, target, count, chosen=None):
    width = edges.shape[1]
    lat = strip.shape[1] // pitch
    lane = lanes_of(strip)
    moves = {}
    for l in range(lat):
        slot = (l + turn) % lat
        moves.setdefault((slot * pitch + target - SLOT * l - source) % width, []).append(slot)
    for shift, slots in moves.items():
        moved = jnp.concatenate([roll(edges, shift)] * (strip.shape[1] // width), axis=1)
        mask = None
        for slot in slots:
            here = between(lane, slot * pitch + target, slot * pitch + target + count)
            mask = here if mask is None else jnp.logical_or(mask, here)
        if chosen is not None:
            mask = jnp.logical_and(mask, chosen)
        strip = jnp.where(mask, moved, strip)
    return strip


def first_kernel(lat, coef_ref, x_ref, n_ref, before_ref, after_ref, column_ref, w_in_ref, w_out_ref, *refs):
    outs = refs[:GROUP]
    (inc_ref,) = refs[GROUP:]
    rows = n_ref.shape[1]
    strip = n_ref.shape[2]
    width = before_ref.shape[1]
    sub = width // GROUP
    pitch = strip // lat
    turn = turn_of(pitch, sub, width)
    _, quarter = place()
    half, drift, spread, time = [coef_ref[r : r + 1, 0:1] for r in range(4)]
    shift = column_ref[...] * time
    before = before_ref[...]
    after = after_ref[...]
    tail = x_ref.shape[1] - rows
    quarters = range(GROUP)
    strips = []
    others = []
    for q in quarters:
        x = x_ref[q, 0:rows]
        noise = n_ref[q]
        if q == 0:
            x = edged(x, before, pitch, turn * q, 0, 0, 4)
            noise = edged(noise, before, pitch, turn * q, 4, 2, 2)
        if q == GROUP - 1:
            x = edged(x, after, pitch, turn * q, 4, pitch - EDGE, 4)
            noise = edged(noise, after, pitch, turn * q, 0, pitch - EDGE, 2)
        strips.append(jnp.concatenate([x, jnp.zeros((tail, strip), F32)], axis=0))
        others.append(x * half + noise * spread)
    firsts = [(turn * q) % lat for q in quarters]
    scores = scores_of(strips, [shift] * GROUP, firsts, w_in_ref, w_out_ref, pitch)
    for q, score, other in zip(quarters, scores, others):
        inc_ref[q] = roll(other + drift * score, -pitch * turn * q)
    for m in range(GROUP):
        outs[m][...] = inc_ref[lax.bitwise_xor(quarter, m)]


def base_kernel(lat, anchor_ref, before_ref, after_ref, *refs):
    incs = refs[:GROUP]
    base_ref, tight_ref, inc_ref, anc_ref = refs[GROUP:]
    chans = anchor_ref.shape[0] // lat
    width = anchor_ref.shape[1]
    sub = width // GROUP
    strip = base_ref.shape[2]
    pitch = strip // lat
    mine, quarter = place()
    for m in range(GROUP):
        inc_ref[lax.bitwise_xor(mine, m)] = incs[m][...]
    anc_ref[chans // ROWS * ROWS :, :] = jnp.zeros_like(anc_ref[chans // ROWS * ROWS :, :])
    tight_ref[chans // ROWS * ROWS :, :] = jnp.zeros_like(tight_ref[chans // ROWS * ROWS :, :])
    turned = []
    for l in range(lat):
        turned.append(pltpu.roll(anchor_ref[pl.ds(l, chans, stride=lat), :], lax.rem(width - quarter * sub, width), 1))
    for t, tile in enumerate(tiled([roll(line, pitch * l + EDGE) for l, line in enumerate(turned)], pitch, 0)):
        anc_ref[0:chans, t * width : (t + 1) * width] = tile
    block = lanes_of(turned[0]) // sub
    for t in range(lat // GROUP):
        tile = turned[GROUP * t]
        for i in range(1, GROUP):
            tile = jnp.where(block == i, roll(turned[GROUP * t + i], i * sub), tile)
        tight_ref[0:chans, t * width : (t + 1) * width] = tile
    state = edged(anc_ref[...], before_ref[...], pitch, 0, 6, 2, 2, quarter == 0)
    state = edged(state, after_ref[...], pitch, 0, 2, pitch - EDGE, 2, quarter == GROUP - 1)
    for j in range(GROUP):
        base_ref[j] = state
        if j + 1 < GROUP:
            state = state + inc_ref[j]


def second_kernel(lat, coef_ref, base_ref, column_ref, w_in_ref, w_out_ref, carry_ref, sum_ref):
    rows, strip = carry_ref.shape
    pitch = strip // lat
    width = coef_ref.shape[1]
    sub = width // GROUP
    tail = w_in_ref.shape[1] // 9 - rows
    carry = carry_ref[...]

    def packed(block):
        tiles = [block[:, t * width : (t + 1) * width] for t in range(strip // width)]
        lane = lanes_of(tiles[0])
        outs = []
        for l in range(lat):
            low = l * pitch + EDGE
            piece = tiles[low // width]
            if (low + sub - 1) // width != low // width:
                piece = jnp.where(lane >= low % width, piece, tiles[low // width + 1])
            moved = roll(piece, (l % GROUP) * sub - low)
            outs.append(moved if l % GROUP == 0 else jnp.where(lane >= (l % GROUP) * sub, moved, outs.pop()))
        return jnp.concatenate(outs, axis=1)

    running = jnp.zeros(sum_ref.shape[1:], F32)
    levels = range(GROUP)
    states = [base_ref[j] + carry for j in levels]
    strips = [jnp.concatenate([x, jnp.zeros((tail, strip), F32)], axis=0) for x in states]
    coefs = [[coef_ref[COEFS * (j + 1) + r : COEFS * (j + 1) + r + 1, 0:1] for r in range(4)] for j in levels]
    shifts = [column_ref[...] * coef[3] for coef in coefs]
    scores = scores_of(strips, shifts, [0] * GROUP, w_in_ref, w_out_ref, pitch)
    for j, x, score, coef in zip(levels, states, scores, coefs):
        running = running + packed(x * coef[0] + score * coef[1])
        sum_ref[j] = running


def share_kernel(tight_ref, sum_ref, *refs):
    waves = refs[:GROUP]
    outs = refs[GROUP : 2 * GROUP]
    total_ref, wave_ref = refs[2 * GROUP :]
    mine, _ = place()
    for m in range(GROUP):
        wave_ref[lax.bitwise_xor(mine, m)] = waves[m][...]
    noise = jnp.zeros(total_ref.shape, F32)
    for j in range(GROUP):
        noise = noise + wave_ref[j]
        share = sum_ref[j] + noise
        wave_ref[j] = tight_ref[...] + share
    total_ref[...] = share
    for m in range(GROUP):
        outs[m][...] = wave_ref[lax.bitwise_xor(mine, m)]


def last_kernel(lat, *refs):
    parts = refs[:GROUP]
    out_any, all_ref, line_ref, sems = refs[GROUP:]
    chans = line_ref.shape[0] // lat
    width = line_ref.shape[1]
    _, quarter = place()
    for m in range(GROUP):
        all_ref[lax.bitwise_xor(quarter, m)] = parts[m][...]
    size = up_to(-(-chans // sems.shape[0]), ROWS)
    copies = []
    for i, low in enumerate(range(0, chans, size)):
        high = min(low + size, chans)
        for t in range(lat // GROUP):
            lanes = slice(t * width, (t + 1) * width)
            lines = swapped([all_ref[q, low:high, lanes] for q in range(GROUP)])
            for k, line in enumerate(lines):
                line_ref[pl.ds(low * lat + GROUP * t + k, high - low, stride=lat), :] = line
        spot = pl.ds(low * lat, (high - low) * lat)
        copies.append(pltpu.make_async_copy(line_ref.at[spot], out_any.at[spot], sems.at[i]))
        copies[-1].start()
    for copy in copies:
        copy.wait()


def exchange(pieces):
    count = lax.axis_size("lvl")
    got = [pieces[0]]
    for m in range(1, GROUP):
        got.append(lax.ppermute(pieces[m], "lvl", [(k, k ^ m) for k in range(count)]))
    return got


def carried(total, block):
    count = lax.axis_size("lvl")
    blocks = count // GROUP
    carry = jnp.zeros_like(total)
    for s in range(1, blocks):
        pairs = []
        for k in range(count):
            target = (k // GROUP + s) % blocks
            turn = (k // GROUP + target) % 2 * (GROUP // 2)
            pairs.append((k, target * GROUP + (k % GROUP ^ turn)))
        moved = lax.ppermute(total, "lvl", pairs)
        carry = carry + jnp.where(block >= s, moved, 0.0)
    return carry


def body(window, anchor, noise, conv_in, conv_out, time_shift, plan, start):
    _, lat, chans, width = window.shape
    hid = conv_in.shape[2]
    block = lax.axis_index("lvl") // GROUP
    sub = width // GROUP
    strip = lat * (sub + 2 * EDGE)
    rows = up_to(chans, ROWS)
    deep = up_to(chans, PACK)

    def native(x):
        return jnp.transpose(x.reshape(lat, chans, width), (1, 0, 2)).reshape(chans * lat, width)

    edge = (rows, SLOT * lat)
    wide = (rows, strip)
    tight = (rows, lat * sub)
    flops = 2 * 9 * chans * hid * 2 * lat * width
    taps = jax.ShapeDtypeStruct((3, 3, chans, hid), BF16)
    first, last, coefs, win, noi, anc, taps_in, taps_out, time = call(
        functools.partial(edges_kernel, lat),
        [edge, edge, (COEFS * (GROUP + 1), width)] + [(chans * lat, width)] * 3 + [taps, taps, (1, hid)],
        [SM] + [HBM] * 7,
        [
            pltpu.SMEM(plan.shape, plan.dtype),
            pltpu.SemaphoreType.DMA((7,)),
        ],
        1 << 20,
        8,
    )(
        start,
        *(
            pltpu.with_memory_space_constraint(x, pltpu.HBM)
            for x in (
                plan,
                native(window),
                native(noise),
                native(anchor),
                jnp.swapaxes(conv_in, 2, 3),
                conv_out,
                time_shift.reshape(1, hid),
            )
        )
    )
    count = lax.axis_size("lon")
    before = lax.ppermute(last, "lon", [(k, (k + 1) % count) for k in range(count)])
    after = lax.ppermute(first, "lon", [((k + 1) % count, k) for k in range(count)])
    w_in, w_out, column, x, n, *waves = call(
        functools.partial(build_kernel, lat),
        [
            jax.ShapeDtypeStruct((hid, 9 * deep), BF16),
            jax.ShapeDtypeStruct((3 * rows, 3 * hid), BF16),
            jax.ShapeDtypeStruct((hid, 1), F32),
            (GROUP, deep, strip),
            (GROUP,) + wide,
        ]
        + [tight] * GROUP,
        [VM] * 6,
        [
            pltpu.VMEM((9 * deep, hid), F32),
            pltpu.VMEM((3 * rows, 3 * hid), F32),
            pltpu.VMEM((GROUP,) + tight, F32),
        ],
        flops // 4,
        12,
    )(coefs, taps_in, taps_out, time, win, noi)
    incs = call(
        functools.partial(first_kernel, lat),
        [wide] * GROUP,
        [VM] * 8,
        [pltpu.VMEM((GROUP,) + wide, F32)],
        flops,
        20,
    )(coefs, x, n, before, after, column, w_in, w_out)
    incs = exchange(incs)
    total = incs[0] + incs[1] + incs[2] + incs[3]
    carry = carried(total, block)
    waves = exchange(waves)
    base, packed = call(
        functools.partial(base_kernel, lat),
        [(GROUP,) + wide, tight],
        [VM] * (3 + GROUP),
        [pltpu.VMEM((GROUP,) + wide, F32), pltpu.VMEM(wide, F32)],
        flops // 4,
        12,
    )(anc, before, after, *incs)
    (sums,) = call(
        functools.partial(second_kernel, lat),
        [(GROUP,) + tight],
        [VM] * 6,
        [],
        flops,
        20,
    )(coefs, base, column, w_in, w_out, carry)
    done = call(
        share_kernel,
        [tight] * (GROUP + 1),
        [VM] * (2 + GROUP),
        [pltpu.VMEM((GROUP,) + tight, F32)],
        1 << 20,
        4,
    )(packed, sums, *waves)
    carry = carried(done[GROUP], block)
    parts = exchange([part + carry for part in done[:GROUP]])
    (out,) = call(
        functools.partial(last_kernel, lat),
        [(chans * lat, width)],
        [VM] * GROUP,
        [pltpu.VMEM((GROUP,) + tight, F32), pltpu.VMEM((chans * lat, width), F32), pltpu.SemaphoreType.DMA((5,))],
        1 << 20,
        8,
        [HBM],
    )(*parts)
    return jnp.transpose(out.reshape(chans, lat, width), (1, 0, 2))[None]


def solution(mesh):
    return jax.shard_map(
        body,
        mesh=mesh,
        in_specs=(
            P("lvl", None, None, "lon"),
            P(None, None, "lon"),
            P("lvl", None, None, "lon"),
            P(),
            P(),
            P(),
            P(),
            P(),
        ),
        out_specs=P("lvl", None, None, "lon"),
        check_vma=False,
    )
```

```python
import functools

import jax
import jax.numpy as jnp
from jax import lax
from jax.experimental import pallas as pl
from jax.experimental.pallas import tpu as pltpu
from jax.sharding import PartitionSpec as P


GROUP = 4
EDGE = 4
SLOT = 2 * EDGE
ROWS = 8
PACK = 16
COEFS = 8

VM = pl.BlockSpec(memory_space=pltpu.VMEM)
SM = pl.BlockSpec(memory_space=pltpu.SMEM)
HBM = pl.BlockSpec(memory_space=pltpu.HBM)
F32 = jnp.float32
BF16 = jnp.bfloat16


def up_to(value, unit):
    return -(-value // unit) * unit


def call(kernel, outs, specs, scratch, flops, limit, out_specs=None):
    outs = [out if isinstance(out, jax.ShapeDtypeStruct) else jax.ShapeDtypeStruct(out, F32) for out in outs]
    return pl.pallas_call(
        kernel,
        out_shape=outs,
        in_specs=specs,
        out_specs=out_specs or [VM] * len(outs),
        scratch_shapes=scratch,
        compiler_params=pltpu.CompilerParams(vmem_limit_bytes=int(limit * (1 << 20))),
        cost_estimate=pl.CostEstimate(flops=flops, bytes_accessed=4 << 20, transcendentals=0),
    )


def roll(x, shift):
    shift = shift % x.shape[1]
    return pltpu.roll(x, shift, 1) if shift else x


def lanes_of(x):
    return lax.broadcasted_iota(jnp.int32, x.shape, 1)


def place():
    level = lax.axis_index("lvl")
    mine = lax.rem(level, GROUP)
    return mine, lax.bitwise_xor(mine, lax.rem(level // GROUP, 2) * (GROUP // 2))


def between(lane, low, high):
    return jnp.logical_and(lane >= low, lane < high)


def swapped(arrays):
    count = len(arrays)
    sub = arrays[0].shape[1] // count
    block = lanes_of(arrays[0]) // sub
    turned = []
    for r in range(count):
        mixed = arrays[r]
        for j in range(1, count):
            mixed = jnp.where(block == j, arrays[(j + r) % count], mixed)
        turned.append(roll(mixed, r * sub))
    outs = []
    for j in range(count):
        mixed = turned[(0 - j) % count]
        for i in range(1, count):
            mixed = jnp.where(block == i, turned[(i - j) % count], mixed)
        outs.append(mixed)
    return outs


def coefs_of(plan_ref, entry):
    now = plan_ref[entry].astype(F32)
    later = plan_ref[entry + 1].astype(F32)
    beta = 0.1 + 19.9 * now / 1000.0
    step = (now - later) / 1000.0
    return [0.5 * beta * step, beta * step, jnp.sqrt(jnp.full((1, 1), beta * step, F32)), now / 1000.0]


def edges_kernel(
    lat, start_ref, plan_hbm, win_hbm, noise_hbm, anchor_hbm, conv_in_hbm, conv_out_hbm, time_hbm,
    first_ref, last_ref, coef_ref, win_ref, noise_ref, anchor_ref, conv_in_ref, conv_out_ref, time_ref,
    plan_ref, sems,
):
    pairs = [
        (plan_hbm, plan_ref),
        (win_hbm, win_ref),
        (noise_hbm, noise_ref),
        (anchor_hbm, anchor_ref),
        (conv_in_hbm, conv_in_ref),
        (conv_out_hbm, conv_out_ref),
        (time_hbm, time_ref),
    ]
    copies = [pltpu.make_async_copy(source, target, sems.at[i]) for i, (source, target) in enumerate(pairs)]
    for copy in copies:
        copy.start()
    copies[0].wait()
    copies = copies[1:]
    level = lax.axis_index("lvl")
    entries = [level] + [level - lax.rem(level, GROUP) + j for j in range(GROUP)]
    for i, entry in enumerate(entries):
        values = coefs_of(plan_ref, start_ref[0] + entry)
        for r, value in enumerate(values):
            coef_ref[COEFS * i + r : COEFS * i + r + 1, :] = jnp.broadcast_to(
                value if r == 2 else jnp.full((1, 1), value, F32), (1, coef_ref.shape[1])
            )
    chans = win_ref.shape[0] // lat
    tiles = []
    for copy, ref, shift, skip in zip(copies, (win_ref, noise_ref, anchor_ref), (4, 6, 8), (0, 0, 6)):
        copy.wait()
        tile = roll(ref[pl.ds(0, chans, stride=lat), :], shift)
        width = tile.shape[1]
        slot = lax.rem(lanes_of(tile) + width - skip, width) // SLOT
        for l in range(1, lat):
            tile = jnp.where(slot == l, roll(ref[pl.ds(l, chans, stride=lat), :], SLOT * l + shift), tile)
        tiles.append(tile)
    win, noise, anchor = tiles
    spot = lax.rem(lanes_of(win), SLOT)
    last = jnp.where(spot < 4, win, jnp.where(spot < 6, noise, anchor))
    first = jnp.where(spot < 2, roll(noise, -6), jnp.where(spot < 4, roll(anchor, -6), win))
    for ref, value in ((first_ref, first), (last_ref, last)):
        ref[...] = jnp.zeros_like(ref)
        ref[0:chans, :] = value
    for copy in copies[3:]:
        copy.wait()


def tiled(rolled, pitch, turn):
    lat = len(rolled)
    width = rolled[0].shape[1]
    lane = lanes_of(rolled[0])
    tiles = []
    for t in range(lat * pitch // width):
        tile = None
        for slot in range(lat):
            low = slot * pitch - t * width
            if low >= width or low + pitch <= 0:
                continue
            piece = rolled[(slot - turn) % lat]
            tile = piece if tile is None else jnp.where(lane >= low, piece, tile)
        tiles.append(tile)
    return tiles


def turn_of(pitch, sub, width):
    return next(k for k in range(width) if (pitch * k) % width == sub)


def build_kernel(
    lat, coef_ref, conv_in_ref, conv_out_ref, time_ref, win_ref, noise_ref,
    w_in_ref, w_out_ref, column_ref, x_ref, n_ref, *refs,
):
    waves = refs[:GROUP]
    in_ref, out_ref, wave_ref = refs[GROUP:]
    chans, hid = conv_in_ref.shape[2:]
    width = win_ref.shape[1]
    deep = in_ref.shape[0] // 9
    rows = n_ref.shape[1]
    sub = width // GROUP
    pitch = sub + 2 * EDGE
    turn = turn_of(pitch, sub, width)
    for source, target in ((win_ref, x_ref), (noise_ref, n_ref)):
        target[:, chans // ROWS * ROWS :, :] = jnp.zeros_like(target[:, chans // ROWS * ROWS :, :])
        rolled = [roll(source[pl.ds(l, chans, stride=lat), :], pitch * l + EDGE) for l in range(lat)]
        for q in range(GROUP):
            for t, tile in enumerate(tiled(rolled, pitch, turn * q)):
                target[q, 0:chans, t * width : (t + 1) * width] = tile
    _, quarter = place()
    in_ref[...] = jnp.zeros_like(in_ref)
    out_ref[...] = jnp.zeros_like(out_ref)
    for b in range(3):
        for a in range(3):
            tap = 3 * b + a
            in_ref[tap * deep : tap * deep + chans, :] = conv_in_ref[a, b].astype(F32)
            out_ref[a * rows : a * rows + chans, b * hid : (b + 1) * hid] = conv_out_ref[a, b].astype(F32)
    w_in_ref[...] = jnp.transpose(in_ref[...]).astype(BF16)
    w_out_ref[...] = out_ref[...].astype(BF16)
    column_ref[...] = jnp.transpose(jnp.broadcast_to(time_ref[...], (ROWS, hid)))[:, :1]

    spread = coef_ref[2:3, 0:1]
    wave_ref[:, chans // ROWS * ROWS :, :] = jnp.zeros_like(wave_ref[:, chans // ROWS * ROWS :, :])
    for t in range(lat // GROUP):
        lines = [noise_ref[pl.ds(GROUP * t + i, chans, stride=lat), :] * spread for i in range(GROUP)]
        for q, line in enumerate(swapped(lines)):
            wave_ref[q, 0:chans, t * width : (t + 1) * width] = line
    for m in range(GROUP):
        waves[m][...] = wave_ref[lax.bitwise_xor(quarter, m)]


def lat_shifted(x, pitch, first):
    lane = lanes_of(x)
    slots = x.shape[1] // pitch
    zero = jnp.zeros_like(x)
    final = (first - 1) % slots
    below = jnp.where(between(lane, first * pitch, (first + 1) * pitch), zero, roll(x, pitch))
    above = jnp.where(between(lane, final * pitch, (final + 1) * pitch), zero, roll(x, -pitch))
    return below, above


def scores_of(strips, shifts, firsts, w_in_ref, w_out_ref, pitch):
    strip = strips[0].shape[1]
    rows = w_out_ref.shape[0] // 3
    stacks = []
    for x, first in zip(strips, firsts):
        x = x.astype(BF16)
        stack = []
        for moved in (roll(x, 1), x, roll(x, -1)):
            below, above = lat_shifted(moved, pitch, first)
            stack += [below, moved, above]
        stacks.append(jnp.concatenate(stack, axis=0))
    pre = jnp.dot(w_in_ref[...], jnp.concatenate(stacks, axis=1), preferred_element_type=F32)
    hiddens = []
    for i, shift in enumerate(shifts):
        value = pre[:, i * strip : (i + 1) * strip] + shift
        hidden = (value / (1.0 + jnp.exp(-value))).astype(BF16)
        hiddens.append(jnp.concatenate([roll(hidden, 1), hidden, roll(hidden, -1)], axis=0))
    out = jnp.dot(w_out_ref[...], jnp.concatenate(hiddens, axis=1), preferred_element_type=F32)
    scores = []
    for i, first in enumerate(firsts):
        lines = out[:, i * strip : (i + 1) * strip]
        below, _ = lat_shifted(lines[:rows], pitch, first)
        _, above = lat_shifted(lines[2 * rows :], pitch, first)
        scores.append(lines[rows : 2 * rows] + below + above)
    return scores


def edged(strip, edges, pitch, turn, source, target, count, chosen=None):
    width = edges.shape[1]
    lat = strip.shape[1] // pitch
    lane = lanes_of(strip)
    moves = {}
    for l in range(lat):
        slot = (l + turn) % lat
        moves.setdefault((slot * pitch + target - SLOT * l - source) % width, []).append(slot)
    for shift, slots in moves.items():
        moved = jnp.concatenate([roll(edges, shift)] * (strip.shape[1] // width), axis=1)
        mask = None
        for slot in slots:
            here = between(lane, slot * pitch + target, slot * pitch + target + count)
            mask = here if mask is None else jnp.logical_or(mask, here)
        if chosen is not None:
            mask = jnp.logical_and(mask, chosen)
        strip = jnp.where(mask, moved, strip)
    return strip


def first_kernel(lat, coef_ref, x_ref, n_ref, before_ref, after_ref, column_ref, w_in_ref, w_out_ref, *refs):
    outs = refs[:GROUP]
    (inc_ref,) = refs[GROUP:]
    rows = n_ref.shape[1]
    strip = n_ref.shape[2]
    width = before_ref.shape[1]
    sub = width // GROUP
    pitch = strip // lat
    turn = turn_of(pitch, sub, width)
    _, quarter = place()
    half, drift, spread, time = [coef_ref[r : r + 1, 0:1] for r in range(4)]
    shift = column_ref[...] * time
    before = before_ref[...]
    after = after_ref[...]
    tail = x_ref.shape[1] - rows
    quarters = range(GROUP)
    strips = []
    others = []
    for q in quarters:
        x = x_ref[q, 0:rows]
        noise = n_ref[q]
        if q == 0:
            x = edged(x, before, pitch, turn * q, 0, 0, 4)
            noise = edged(noise, before, pitch, turn * q, 4, 2, 2)
        if q == GROUP - 1:
            x = edged(x, after, pitch, turn * q, 4, pitch - EDGE, 4)
            noise = edged(noise, after, pitch, turn * q, 0, pitch - EDGE, 2)
        strips.append(jnp.concatenate([x, jnp.zeros((tail, strip), F32)], axis=0))
        others.append(x * half + noise * spread)
    firsts = [(turn * q) % lat for q in quarters]
    scores = scores_of(strips, [shift] * GROUP, firsts, w_in_ref, w_out_ref, pitch)
    for q, score, other in zip(quarters, scores, others):
        inc_ref[q] = roll(other + drift * score, -pitch * turn * q)
    for m in range(GROUP):
        outs[m][...] = inc_ref[lax.bitwise_xor(quarter, m)]


def base_kernel(lat, anchor_ref, before_ref, after_ref, *refs):
    incs = refs[:GROUP]
    base_ref, tight_ref, inc_ref, anc_ref = refs[GROUP:]
    chans = anchor_ref.shape[0] // lat
    width = anchor_ref.shape[1]
    sub = width // GROUP
    strip = base_ref.shape[2]
    pitch = strip // lat
    mine, quarter = place()
    for m in range(GROUP):
        inc_ref[lax.bitwise_xor(mine, m)] = incs[m][...]
    anc_ref[chans // ROWS * ROWS :, :] = jnp.zeros_like(anc_ref[chans // ROWS * ROWS :, :])
    tight_ref[chans // ROWS * ROWS :, :] = jnp.zeros_like(tight_ref[chans // ROWS * ROWS :, :])
    turned = []
    for l in range(lat):
        turned.append(pltpu.roll(anchor_ref[pl.ds(l, chans, stride=lat), :], lax.rem(width - quarter * sub, width), 1))
    for t, tile in enumerate(tiled([roll(line, pitch * l + EDGE) for l, line in enumerate(turned)], pitch, 0)):
        anc_ref[0:chans, t * width : (t + 1) * width] = tile
    block = lanes_of(turned[0]) // sub
    for t in range(lat // GROUP):
        tile = turned[GROUP * t]
        for i in range(1, GROUP):
            tile = jnp.where(block == i, roll(turned[GROUP * t + i], i * sub), tile)
        tight_ref[0:chans, t * width : (t + 1) * width] = tile
    state = edged(anc_ref[...], before_ref[...], pitch, 0, 6, 2, 2, quarter == 0)
    state = edged(state, after_ref[...], pitch, 0, 2, pitch - EDGE, 2, quarter == GROUP - 1)
    for j in range(GROUP):
        base_ref[j] = state
        if j + 1 < GROUP:
            state = state + inc_ref[j]


def second_kernel(lat, coef_ref, base_ref, column_ref, w_in_ref, w_out_ref, carry_ref, sum_ref):
    rows, strip = carry_ref.shape
    pitch = strip // lat
    width = coef_ref.shape[1]
    sub = width // GROUP
    tail = w_in_ref.shape[1] // 9 - rows
    carry = carry_ref[...]

    def packed(block):
        tiles = [block[:, t * width : (t + 1) * width] for t in range(strip // width)]
        lane = lanes_of(tiles[0])
        outs = []
        for l in range(lat):
            low = l * pitch + EDGE
            piece = tiles[low // width]
            if (low + sub - 1) // width != low // width:
                piece = jnp.where(lane >= low % width, piece, tiles[low // width + 1])
            moved = roll(piece, (l % GROUP) * sub - low)
            outs.append(moved if l % GROUP == 0 else jnp.where(lane >= (l % GROUP) * sub, moved, outs.pop()))
        return jnp.concatenate(outs, axis=1)

    running = jnp.zeros(sum_ref.shape[1:], F32)
    levels = range(GROUP)
    states = [base_ref[j] + carry for j in levels]
    strips = [jnp.concatenate([x, jnp.zeros((tail, strip), F32)], axis=0) for x in states]
    coefs = [[coef_ref[COEFS * (j + 1) + r : COEFS * (j + 1) + r + 1, 0:1] for r in range(4)] for j in levels]
    shifts = [column_ref[...] * coef[3] for coef in coefs]
    scores = scores_of(strips, shifts, [0] * GROUP, w_in_ref, w_out_ref, pitch)
    for j, x, score, coef in zip(levels, states, scores, coefs):
        running = running + packed(x * coef[0] + score * coef[1])
        sum_ref[j] = running


def share_kernel(tight_ref, sum_ref, *refs):
    waves = refs[:GROUP]
    outs = refs[GROUP : 2 * GROUP]
    (wave_ref,) = refs[2 * GROUP :]
    mine, _ = place()
    for m in range(GROUP):
        wave_ref[lax.bitwise_xor(mine, m)] = waves[m][...]
    noise = jnp.zeros(tight_ref.shape, F32)
    for j in range(GROUP):
        noise = noise + wave_ref[j]
        wave_ref[j] = tight_ref[...] + (sum_ref[j] + noise)
    for m in range(GROUP):
        outs[m][...] = wave_ref[lax.bitwise_xor(mine, m)]


def last_kernel(lat, *refs):
    parts = refs[:GROUP]
    out_any, all_ref, line_ref, sems = refs[GROUP:]
    chans = line_ref.shape[0] // lat
    width = line_ref.shape[1]
    _, quarter = place()
    for m in range(GROUP):
        all_ref[lax.bitwise_xor(quarter, m)] = parts[m][...]
    size = up_to(-(-chans // sems.shape[0]), ROWS)
    copies = []
    for i, low in enumerate(range(0, chans, size)):
        high = min(low + size, chans)
        for t in range(lat // GROUP):
            lanes = slice(t * width, (t + 1) * width)
            lines = swapped([all_ref[q, low:high, lanes] for q in range(GROUP)])
            for k, line in enumerate(lines):
                line_ref[pl.ds(low * lat + GROUP * t + k, high - low, stride=lat), :] = line
        spot = pl.ds(low * lat, (high - low) * lat)
        copies.append(pltpu.make_async_copy(line_ref.at[spot], out_any.at[spot], sems.at[i]))
        copies[-1].start()
    for copy in copies:
        copy.wait()


def exchange(pieces):
    count = lax.axis_size("lvl")
    got = [pieces[0]]
    for m in range(1, GROUP):
        got.append(lax.ppermute(pieces[m], "lvl", [(k, k ^ m) for k in range(count)]))
    return got


def carried(total, block):
    count = lax.axis_size("lvl")
    blocks = count // GROUP
    carry = jnp.zeros_like(total)
    for s in range(1, blocks):
        pairs = []
        for k in range(count):
            target = (k // GROUP + s) % blocks
            turn = (k // GROUP + target) % 2 * (GROUP // 2)
            pairs.append((k, target * GROUP + (k % GROUP ^ turn)))
        moved = lax.ppermute(total, "lvl", pairs)
        carry = carry + jnp.where(block >= s, moved, 0.0)
    return carry


def body(window, anchor, noise, conv_in, conv_out, time_shift, plan, start):
    _, lat, chans, width = window.shape
    hid = conv_in.shape[2]
    block = lax.axis_index("lvl") // GROUP
    sub = width // GROUP
    strip = lat * (sub + 2 * EDGE)
    rows = up_to(chans, ROWS)
    deep = up_to(chans, PACK)

    def native(x):
        return jnp.transpose(x.reshape(lat, chans, width), (1, 0, 2)).reshape(chans * lat, width)

    edge = (rows, SLOT * lat)
    wide = (rows, strip)
    tight = (rows, lat * sub)
    flops = 2 * 9 * chans * hid * 2 * lat * width
    taps = jax.ShapeDtypeStruct((3, 3, chans, hid), BF16)
    first, last, coefs, win, noi, anc, taps_in, taps_out, time = call(
        functools.partial(edges_kernel, lat),
        [edge, edge, (COEFS * (GROUP + 1), width)] + [(chans * lat, width)] * 3 + [taps, taps, (1, hid)],
        [SM] + [HBM] * 7,
        [
            pltpu.SMEM(plan.shape, plan.dtype),
            pltpu.SemaphoreType.DMA((7,)),
        ],
        1 << 20,
        8,
    )(
        start,
        *(
            pltpu.with_memory_space_constraint(x, pltpu.HBM)
            for x in (
                plan,
                native(window),
                native(noise),
                native(anchor),
                jnp.swapaxes(conv_in, 2, 3),
                conv_out,
                time_shift.reshape(1, hid),
            )
        )
    )
    count = lax.axis_size("lon")
    before = lax.ppermute(last, "lon", [(k, (k + 1) % count) for k in range(count)])
    after = lax.ppermute(first, "lon", [((k + 1) % count, k) for k in range(count)])
    w_in, w_out, column, x, n, *waves = call(
        functools.partial(build_kernel, lat),
        [
            jax.ShapeDtypeStruct((hid, 9 * deep), BF16),
            jax.ShapeDtypeStruct((3 * rows, 3 * hid), BF16),
            jax.ShapeDtypeStruct((hid, 1), F32),
            (GROUP, deep, strip),
            (GROUP,) + wide,
        ]
        + [tight] * GROUP,
        [VM] * 6,
        [
            pltpu.VMEM((9 * deep, hid), F32),
            pltpu.VMEM((3 * rows, 3 * hid), F32),
            pltpu.VMEM((GROUP,) + tight, F32),
        ],
        flops // 4,
        12,
    )(coefs, taps_in, taps_out, time, win, noi)
    incs = call(
        functools.partial(first_kernel, lat),
        [wide] * GROUP,
        [VM] * 8,
        [pltpu.VMEM((GROUP,) + wide, F32)],
        flops,
        20,
    )(coefs, x, n, before, after, column, w_in, w_out)
    incs = exchange(incs)
    total = incs[0] + incs[1] + incs[2] + incs[3]
    carry = carried(total, block)
    waves = exchange(waves)
    base, packed = call(
        functools.partial(base_kernel, lat),
        [(GROUP,) + wide, tight],
        [VM] * (3 + GROUP),
        [pltpu.VMEM((GROUP,) + wide, F32), pltpu.VMEM(wide, F32)],
        flops // 4,
        12,
    )(anc, before, after, *incs)
    (sums,) = call(
        functools.partial(second_kernel, lat),
        [(GROUP,) + tight],
        [VM] * 6,
        [],
        flops,
        20,
    )(coefs, base, column, w_in, w_out, carry)
    carry = carried(sums[GROUP - 1] + (waves[0] + waves[1] + waves[2] + waves[3]), block)
    done = call(
        share_kernel,
        [tight] * GROUP,
        [VM] * (2 + GROUP),
        [pltpu.VMEM((GROUP,) + tight, F32)],
        flops // 4,
        4,
    )(packed, sums, *waves)
    parts = exchange([part + carry for part in done])
    (out,) = call(
        functools.partial(last_kernel, lat),
        [(chans * lat, width)],
        [VM] * GROUP,
        [pltpu.VMEM((GROUP,) + tight, F32), pltpu.VMEM((chans * lat, width), F32), pltpu.SemaphoreType.DMA((5,))],
        1 << 20,
        8,
        [HBM],
    )(*parts)
    return jnp.transpose(out.reshape(chans, lat, width), (1, 0, 2))[None]


def solution(mesh):
    return jax.shard_map(
        body,
        mesh=mesh,
        in_specs=(
            P("lvl", None, None, "lon"),
            P(None, None, "lon"),
            P("lvl", None, None, "lon"),
            P(),
            P(),
            P(),
            P(),
            P(),
        ),
        out_specs=P("lvl", None, None, "lon"),
        check_vma=False,
    )
```
